8 devices in a mesh: dp: 1 (over z), tp: 8 (over y, x, core).
Axes of the slice: x: 2, y: 2, z: 1, core: 2. Of those that a mesh axis runs over, the one named last changes fastest.
Arguments:
- x: bfloat16 [256, 2048], P('dp')
- cache_len: int32 [256], P('dp')
- k_cache: bfloat16 [2, 256, 32, 128, 64], P(None, 'dp', 'tp')
- v_cache: bfloat16 [2, 256, 32, 128, 64], P(None, 'dp', 'tp')
- norm_gain: float32 [2, 2, 2048], replicated
- norm_bias: float32 [2, 2, 2048], replicated
- w_qkv: bfloat16 [2, 2048, 3, 32, 64], P(None, None, None, 'tp')
- b_qkv: bfloat16 [2, 3, 32, 64], P(None, None, 'tp')
- w_out: bfloat16 [2, 32, 64, 2048], P(None, 'tp')
- b_out: bfloat16 [2, 2048], replicated
- w_up: bfloat16 [2, 2048, 8192], P(None, None, 'tp')
- b_up: bfloat16 [2, 8192], P(None, 'tp')
- w_down: bfloat16 [2, 8192, 2048], P(None, 'tp')
- b_down: bfloat16 [2, 2048], replicated
Outputs:
- output 1: bfloat16 [256, 2048], P('dp')
- output 2: bfloat16 [2, 256, 32, 128, 64], P(None, 'dp', 'tp')
- output 3: bfloat16 [2, 256, 32, 128, 64], P(None, 'dp', 'tp')
All inputs are finite; a program needn't handle non-finite values.
Results may differ from the reference program's by a relative error of at most 0.0166233.
Values are sent between devices in bfloat16 or wider.
A program may use at most 1 GiB of HBM per device.

```python
import jax
import jax.numpy as jnp
from jax import lax

D = 2048
HEADS = 32
HEAD = 64
BATCH = 256
SMAX = 128
LAYERS = 2
FFN = 8192
NORM_EPS = 1e-5


def setup_inputs(seed: int = 0, part: int = 0) -> dict:
    part_keys = jax.random.split(jax.random.fold_in(jax.random.key(seed), part), 5)
    shared_keys = jax.random.split(jax.random.key(seed + 1), 10)
    x = jax.random.normal(part_keys[0], (BATCH, D), jnp.float32)
    raw_len = jax.random.randint(part_keys[1], (BATCH,), 0, SMAX)
    full_row = jax.random.randint(part_keys[2], (), 0, BATCH)
    cache_len = jnp.where(jnp.arange(BATCH) == full_row, SMAX - 1, raw_len).astype(jnp.int32)
    cache_shape = (LAYERS, BATCH, HEADS, SMAX, HEAD)
    k_cache = 1.5 * jax.random.normal(part_keys[3], cache_shape, jnp.float32)
    v_cache = jax.random.normal(part_keys[4], cache_shape, jnp.float32)
    norm_gain = 1.0 + 0.3 * jax.random.normal(shared_keys[0], (LAYERS, 2, D), jnp.float32)
    norm_bias = 0.3 * jax.random.normal(shared_keys[1], (LAYERS, 2, D), jnp.float32)
    w_qkv = jax.random.normal(shared_keys[2], (LAYERS, D, 3, HEADS, HEAD), jnp.float32) * D ** -0.5
    b_qkv = 0.5 * jax.random.normal(shared_keys[3], (LAYERS, 3, HEADS, HEAD), jnp.float32)
    w_out = jax.random.normal(shared_keys[4], (LAYERS, HEADS, HEAD, D), jnp.float32) * (HEADS * HEAD) ** -0.5
    b_out = 0.3 * jax.random.normal(shared_keys[5], (LAYERS, D), jnp.float32)
    w_up = jax.random.normal(shared_keys[6], (LAYERS, D, FFN), jnp.float32) * D ** -0.5
    b_up = 0.5 * jax.random.normal(shared_keys[7], (LAYERS, FFN), jnp.float32)
    w_down = jax.random.normal(shared_keys[8], (LAYERS, FFN, D), jnp.float32) * FFN ** -0.5
    b_down = 0.3 * jax.random.normal(shared_keys[9], (LAYERS, D), jnp.float32)
    return {
        'x': x.astype(jnp.bfloat16),
        'cache_len': cache_len,
        'k_cache': k_cache.astype(jnp.bfloat16),
        'v_cache': v_cache.astype(jnp.bfloat16),
        'norm_gain': norm_gain,
        'norm_bias': norm_bias,
        'w_qkv': w_qkv.astype(jnp.bfloat16),
        'b_qkv': b_qkv.astype(jnp.bfloat16),
        'w_out': w_out.astype(jnp.bfloat16),
        'b_out': b_out.astype(jnp.bfloat16),
        'w_up': w_up.astype(jnp.bfloat16),
        'b_up': b_up.astype(jnp.bfloat16),
        'w_down': w_down.astype(jnp.bfloat16),
        'b_down': b_down.astype(jnp.bfloat16),
    }


def layer_norm(vec, gain_vec, bias_vec):
    vec_f = vec.astype(jnp.float32)
    row_mean = jnp.mean(vec_f, axis=-1, keepdims=True)
    centered = vec_f - row_mean
    row_var = jnp.mean(centered * centered, axis=-1, keepdims=True)
    return (centered * lax.rsqrt(row_var + NORM_EPS) * gain_vec + bias_vec).astype(jnp.bfloat16)


def row_attention(row_args):
    q_row, k_row, v_row, kc_row, vc_row, len_row = row_args
    kc_new = lax.dynamic_update_slice_in_dim(kc_row, k_row[:, None, :], len_row, axis=1)
    vc_new = lax.dynamic_update_slice_in_dim(vc_row, v_row[:, None, :], len_row, axis=1)
    scores = jnp.einsum('hd,hjd->hj', q_row.astype(jnp.float32), kc_new.astype(jnp.float32)) * (HEAD ** -0.5)
    visible = jnp.arange(SMAX)[None, :] <= len_row
    scores = jnp.where(visible, scores, -1e30)
    attn_prob = jax.nn.softmax(scores, axis=-1).astype(jnp.bfloat16)
    attended = jnp.einsum('hj,hjd->hd', attn_prob.astype(jnp.float32), vc_new.astype(jnp.float32)).astype(jnp.bfloat16)
    return attended, kc_new, vc_new


def decoder_layer(x, cache_len, layer_par):
    gain_pair, bias_pair, w_qkv, b_qkv, w_out, b_out, w_up, b_up, w_down, b_down, kc_layer, vc_layer = layer_par
    hidden = layer_norm(x, gain_pair[0], bias_pair[0])
    qkv_flat = jnp.dot(hidden, w_qkv.reshape(D, 3 * HEADS * HEAD), preferred_element_type=jnp.float32)
    qkv_all = (qkv_flat.reshape(BATCH, 3, HEADS, HEAD) + b_qkv.astype(jnp.float32)).astype(jnp.bfloat16)
    attended, kc_new, vc_new = lax.map(row_attention, (qkv_all[:, 0], qkv_all[:, 1], qkv_all[:, 2], kc_layer, vc_layer, cache_len))
    attn_sum = jnp.dot(attended.reshape(BATCH, HEADS * HEAD), w_out.reshape(HEADS * HEAD, D), preferred_element_type=jnp.float32)
    x_mid = (x.astype(jnp.float32) + attn_sum + b_out.astype(jnp.float32)).astype(jnp.bfloat16)
    hidden_mlp = layer_norm(x_mid, gain_pair[1], bias_pair[1])
    up_act = jnp.maximum(jnp.dot(hidden_mlp, w_up, preferred_element_type=jnp.float32) + b_up.astype(jnp.float32), 0.0).astype(jnp.bfloat16)
    mlp_sum = jnp.dot(up_act, w_down, preferred_element_type=jnp.float32)
    x_new = (x_mid.astype(jnp.float32) + mlp_sum + b_down.astype(jnp.float32)).astype(jnp.bfloat16)
    return x_new, (kc_new, vc_new)


def reference(x, cache_len, k_cache, v_cache, norm_gain, norm_bias, w_qkv, b_qkv, w_out, b_out, w_up, b_up, w_down, b_down):
    def layer_step(carry, layer_par):
        return decoder_layer(carry, cache_len, layer_par)
    x_final, caches = lax.scan(layer_step, x, (norm_gain, norm_bias, w_qkv, b_qkv, w_out, b_out, w_up, b_up, w_down, b_down, k_cache, v_cache))
    return x_final, caches[0], caches[1]
```

```python
import functools

import jax
import jax.numpy as jnp
from jax import lax
from jax.experimental import pallas as pl
from jax.experimental.pallas import tpu as pltpu
from jax.sharding import PartitionSpec as P

NORM_EPS = 1e-5
MESH = pl.DeviceIdType.MESH
F32 = jnp.float32
BF16 = jnp.bfloat16
NT = (((1,), (1,)), ((), ()))
NN = (((1,), (0,)), ((), ()))

GROUP = 16
CHUNKS = 2


def dot(lhs, rhs, dims=NN):
    return lax.dot_general(lhs, rhs, dims, preferred_element_type=F32)


def norm(rows, gain, bias):
    mean = jnp.mean(rows, axis=-1, keepdims=True)
    centered = rows - mean
    var = jnp.mean(centered * centered, axis=-1, keepdims=True)
    return centered * lax.rsqrt(var + NORM_EPS) * gain + bias


def attention_kernel(layer, lens, x_ref, gain_ref, bias_ref, bqkv_ref, wqkv_hbm, wout_hbm, k_hbm, v_hbm, *rest):
    if layer > 0:
        rest = rest[2:]
    (ko_hbm, vo_hbm, part_ref, kbuf, vbuf, wqkv, wout, hbuf, ktb, vtb, qbuf, abuf,
     w_sem, k_sem, v_sem, ko_sem, vo_sem) = rest
    batch, width = x_ref.shape
    hd = wout.shape[0]
    head = hd // 4
    slots = kbuf.shape[2]
    groups = batch // GROUP

    w_copy = pltpu.make_async_copy(wqkv_hbm.at[layer], wqkv, w_sem.at[0])
    w_copy.start()

    def load(src, buf, sem, g):
        rows = pl.ds(g * GROUP, GROUP)
        return pltpu.make_async_copy(src.at[layer, rows], buf.at[rows], sem.at[g])

    def save(buf, dst, sem, g):
        rows = pl.ds(g * GROUP, GROUP)
        return pltpu.make_async_copy(buf.at[rows], dst.at[layer, rows], sem.at[g])

    def start_loads(g, carry):
        load(k_hbm, kbuf, k_sem, g).start()
        load(v_hbm, vbuf, v_sem, g).start()
        return carry

    lax.fori_loop(0, groups, start_loads, 0)
    o_copy = pltpu.make_async_copy(wout_hbm.at[layer], wout, w_sem.at[1])
    o_copy.start()

    if layer == 0:
        gain = gain_ref[0:1, :]
        bias = bias_ref[0:1, :]

        def norm_rows(i, carry):
            rows = pl.ds(i * 32, 32)
            hbuf[rows, :] = norm(x_ref[rows, :].astype(F32), gain, bias).astype(BF16)
            return carry

        lax.fori_loop(0, batch // 32, norm_rows, 0)
    else:
        hbuf[...] = x_ref[...]
    w_copy.wait()
    hidden = hbuf[...]
    qbuf[...] = (dot(hidden, wqkv[0:hd, :], NT) + bqkv_ref[layer:layer + 1, 0:hd].astype(F32)).astype(BF16)
    for part, pages in ((1, ktb), (2, vtb)):
        row = bqkv_ref[layer:layer + 1, part * hd:(part + 1) * hd].astype(F32)
        column = jnp.broadcast_to(row, (128, hd)).T
        for half in range(batch // 128):
            cols = dot(wqkv[part * hd:(part + 1) * hd, :], hbuf[half * 128:(half + 1) * 128, :], NT) + column
            for j in range(128 // GROUP):
                turned = cols if j == 0 else pltpu.roll(cols, 128 - j * GROUP, 1)
                pages[half * (128 // GROUP) + j] = turned.astype(BF16)

    n = GROUP * 4
    lane8 = lax.broadcasted_iota(jnp.int32, (8, slots), 1)
    top8 = lax.broadcasted_iota(jnp.int32, (8, slots), 0) < 4
    lane_hd = lax.broadcasted_iota(jnp.int32, (hd, slots), 1)
    own_head = (lax.broadcasted_iota(jnp.int32, (n, hd), 0) % 4) == (lax.broadcasted_iota(jnp.int32, (n, hd), 1) // head)
    repeat = ((lax.broadcasted_iota(jnp.int32, (n, GROUP), 0) // 4) == lax.broadcasted_iota(jnp.int32, (n, GROUP), 1)).astype(F32).astype(BF16)
    gather = ((lax.broadcasted_iota(jnp.int32, (GROUP, n), 1) // 4) == lax.broadcasted_iota(jnp.int32, (GROUP, n), 0)).astype(F32).astype(BF16)
    scale = head ** -0.5

    def step(g, carry):
        base = g * GROUP
        rows = pl.ds(pl.multiple_of(base, GROUP), GROUP)
        qrep = jnp.where(own_head, dot(repeat, qbuf[rows, :]), 0.0).astype(BF16)
        load(k_hbm, kbuf, k_sem, g).wait()
        kt = ktb[g].astype(F32)
        probs = []
        for i in range(0, GROUP, 2):
            tiles = []
            for b in (i, i + 1):
                column = jnp.broadcast_to(kt[:, b:b + 1], (hd, slots)).astype(BF16)
                tile = jnp.where(lane_hd == lens[base + b], column, kbuf[base + b])
                kbuf[base + b] = tile
                tiles.append(tile)
            both = dot(qrep[i * 4:i * 4 + 8, :], jnp.concatenate(tiles, axis=1))
            score = jnp.where(top8, both[:, 0:slots], both[:, slots:2 * slots]) * scale
            limit = jnp.where(top8, lens[base + i], lens[base + i + 1])
            probs.append(jnp.where(lane8 <= limit, score, -1e30))
        save(kbuf, ko_hbm, ko_sem, g).start()
        scores = jnp.concatenate(probs, axis=0)
        top = jnp.max(scores, axis=-1, keepdims=True)
        weights = jnp.exp(scores - top)
        prob = weights / jnp.sum(weights, axis=-1, keepdims=True)
        load(v_hbm, vbuf, v_sem, g).wait()
        vt = vtb[g].astype(F32)
        outs = []
        for i in range(0, GROUP, 2):
            tiles = []
            for b in (i, i + 1):
                column = jnp.broadcast_to(vt[:, b:b + 1], (hd, slots)).astype(BF16)
                tile = jnp.where(lane_hd == lens[base + b], column, vbuf[base + b])
                vbuf[base + b] = tile
                tiles.append(tile)
            pair = prob[i * 4:i * 4 + 8, :]
            spread = jnp.concatenate([jnp.where(top8, pair, 0.0), jnp.where(top8, 0.0, pair)], axis=1).astype(BF16)
            outs.append(dot(spread, jnp.concatenate(tiles, axis=1), NT))
        save(vbuf, vo_hbm, vo_sem, g).start()
        heads = jnp.where(own_head, jnp.concatenate(outs, axis=0), 0.0).astype(BF16)
        abuf[rows, :] = dot(gather, heads).astype(BF16)
        return carry

    lax.fori_loop(0, groups, step, 0)
    o_copy.wait()
    part_ref[...] = dot(abuf[...], wout[...]).astype(BF16)

    def finish(g, carry):
        save(kbuf, ko_hbm, ko_sem, g).wait()
        save(vbuf, vo_hbm, vo_sem, g).wait()
        return carry

    lax.fori_loop(0, groups, finish, 0)


def attention(layer, lens, x, gains, biases, bqkv, wqkv, wout, k_in, v_in, k_out=None, v_out=None):
    batch, width = x.shape
    hd = wout.shape[1]
    slots = k_in.shape[3]
    groups = batch // GROUP
    any_spec = pl.BlockSpec(memory_space=pl.ANY)
    vmem_spec = pl.BlockSpec(memory_space=pltpu.VMEM)
    args = [lens, x, gains, biases, bqkv, wqkv, wout, k_in, v_in]
    specs = [pl.BlockSpec(memory_space=pltpu.SMEM)] + [vmem_spec] * 4 + [any_spec] * 4
    alias = {}
    if layer > 0:
        args += [k_out, v_out]
        specs += [any_spec] * 2
        alias = {9: 0, 10: 1}
    return pl.pallas_call(
        functools.partial(attention_kernel, layer),
        out_shape=(
            jax.ShapeDtypeStruct(k_in.shape, BF16),
            jax.ShapeDtypeStruct(v_in.shape, BF16),
            jax.ShapeDtypeStruct((batch, width), BF16),
        ),
        in_specs=specs,
        out_specs=(any_spec, any_spec, vmem_spec),
        input_output_aliases=alias,
        scratch_shapes=[
            pltpu.VMEM((batch, hd, slots), BF16),
            pltpu.VMEM((batch, hd, slots), BF16),
            pltpu.VMEM((3 * hd, width), BF16),
            pltpu.VMEM((hd, width), BF16),
            pltpu.VMEM((batch, width), BF16),
            pltpu.VMEM((groups, hd, 128), BF16),
            pltpu.VMEM((groups, hd, 128), BF16),
            pltpu.VMEM((batch, hd), BF16),
            pltpu.VMEM((batch, hd), BF16),
            pltpu.SemaphoreType.DMA((2,)),
            pltpu.SemaphoreType.DMA((groups,)),
            pltpu.SemaphoreType.DMA((groups,)),
            pltpu.SemaphoreType.DMA((groups,)),
            pltpu.SemaphoreType.DMA((groups,)),
        ],
        compiler_params=pltpu.CompilerParams(vmem_limit_bytes=60 * 1024 * 1024),
        name=f"attention_{layer}",
    )(*args)


def mlp_kernel(layer, last, part_ref, x_ref, gain_ref, bias_ref, bout_ref, bup_ref, bdown_ref, wup_hbm, wdown_hbm,
               full_ref, own_ref, wup, wdown, part2, hbuf, ubuf, pair_in, cross_out, cross_in, own_sum, xown,
               w_sem, pair_s, pair_r, cross_s, cross_r, gat_s, gat_r, fwd_s, fwd_r):
    batch, width = part_ref.shape
    hidden = wup.shape[1]
    rows_c = batch // CHUNKS
    rows_o = rows_c // 8
    me = lax.axis_index("tp")
    core = lax.rem(me, 2)
    chip = lax.div(me, 2)
    cx = lax.rem(chip, 2)
    cy = lax.div(chip, 2)
    partner = chip * 2 + 1 - core
    chips = ((1 - cy) * 2 + 1 - cx, cy * 2 + 1 - cx, (1 - cy) * 2 + cx, chip)

    def device(index):
        return {"tp": index}

    def rows_of(c, owner):
        return pl.ds(pl.multiple_of(c * rows_c + owner * rows_o, rows_o), rows_o)

    copies = [
        pltpu.make_async_copy(wup_hbm.at[layer], wup, w_sem.at[0]),
        pltpu.make_async_copy(wdown_hbm.at[layer], wdown, w_sem.at[1]),
    ]
    for copy in copies:
        copy.start()
    if layer == 0:
        x_copies = [pltpu.make_async_copy(x_ref.at[rows_of(c, me)], xown.at[c], w_sem.at[2 + c]) for c in range(CHUNKS)]
        for copy in x_copies:
            copy.start()

    barrier = pltpu.get_barrier_semaphore()
    for peer in (partner,) + tuple(t * 2 + core for t in chips[:3]):
        pl.semaphore_signal(barrier, inc=1, device_id=device(peer), device_id_type=MESH)
    pl.semaphore_wait(barrier, 4)

    def remote(src, dst, send, recv, target):
        return pltpu.make_async_remote_copy(
            src_ref=src, dst_ref=dst, send_sem=send, recv_sem=recv, device_id=device(target), device_id_type=MESH)

    def pair_copy(s, c, k):
        src = part_ref if s == 0 else part2
        return remote(src.at[rows_of(c, chips[k] * 2 + 1 - core)], pair_in.at[s, c, k],
                      pair_s.at[s, c, k], pair_r.at[s, c, k], partner)

    def cross_copy(s, c, k):
        return remote(cross_out.at[s, c, k], cross_in.at[s, c, k],
                      cross_s.at[s, c, k], cross_r.at[s, c, k], chips[k] * 2 + core)

    def gather_copy(s, c, k):
        rows = rows_of(c, me)
        target = partner if k == 3 else chips[k] * 2 + core
        return remote(hbuf.at[s, rows], hbuf.at[s, rows], gat_s.at[s, c, k], gat_r.at[s, c, k], target)

    def forward_copy(s, c, k):
        rows = rows_of(c, chips[k] * 2 + core)
        return remote(hbuf.at[s, rows], hbuf.at[s, rows], fwd_s.at[s, c, k], fwd_r.at[s, c, k], partner)

    def send_pairs(s, c):
        for k in range(4):
            pair_copy(s, c, k).start()

    def add_pairs(s, c):
        src = part_ref if s == 0 else part2
        for k in range(4):
            pair_copy(s, c, k).wait_recv()
            both = src[rows_of(c, chips[k] * 2 + core), :].astype(F32) + pair_in[s, c, k].astype(F32)
            if k < 3:
                cross_out[s, c, k] = both.astype(BF16)
                cross_copy(s, c, k).start()
            else:
                own_sum[c] = both

    def own_total(s, c):
        total = own_sum[c]
        for k in (1, 2, 0):
            cross_copy(s, c, k).wait_recv()
            total = total + cross_in[s, c, k].astype(F32)
        return total

    def send_own(s, c):
        for k in range(4):
            gather_copy(s, c, k).start()

    def forward(s, c):
        for k in (1, 2, 0):
            gather_copy(s, c, k).wait_recv()
            forward_copy(s, c, k).start()

    def arrived(s, c):
        gather_copy(s, c, 3).wait_recv()
        for k in range(3):
            forward_copy(s, c, k).wait_recv()

    def row(ref, index):
        return ref[index:index + 1, :].astype(F32)

    def first_finish(c):
        total = own_total(0, c)
        old = xown[c] if layer == 0 else x_ref[c]
        mid = (old.astype(F32) + total + row(bout_ref, layer)).astype(BF16)
        xown[c] = mid
        hbuf[0, rows_of(c, me), :] = norm(mid.astype(F32), row(gain_ref, 2 * layer + 1), row(bias_ref, 2 * layer + 1)).astype(BF16)
        send_own(0, c)

    def second_finish(c):
        total = own_total(1, c)
        new = (xown[c].astype(F32) + total + row(bdown_ref, layer)).astype(BF16)
        if last:
            hbuf[1, rows_of(c, me), :] = new
        else:
            own_ref[c] = new
            hbuf[1, rows_of(c, me), :] = norm(new.astype(F32), row(gain_ref, 2 * layer + 2), row(bias_ref, 2 * layer + 2)).astype(BF16)
        send_own(1, c)

    def mlp(c):
        rows = slice(c * rows_c, (c + 1) * rows_c)
        h = hbuf[0, rows, :]
        for n in range(0, hidden, 256):
            up = dot(h, wup[:, n:n + 256]) + bup_ref[layer:layer + 1, n:n + 256].astype(F32)
            ubuf[:, n:n + 256] = jnp.maximum(up, 0.0).astype(BF16)
        u = ubuf[...]
        for n in range(0, width, 256):
            part2[rows, n:n + 256] = dot(u, wdown[:, n:n + 256]).astype(BF16)

    for c in range(CHUNKS):
        send_pairs(0, c)
    for c in range(CHUNKS):
        add_pairs(0, c)
    if layer == 0:
        for copy in x_copies:
            copy.wait()
    for c in range(CHUNKS):
        first_finish(c)
    for copy in copies:
        copy.wait()
    for c in range(CHUNKS):
        forward(0, c)
        if c > 0:
            add_pairs(1, c - 1)
        arrived(0, c)
        mlp(c)
        send_pairs(1, c)
    add_pairs(1, CHUNKS - 1)
    for c in range(CHUNKS):
        second_finish(c)
    for c in range(CHUNKS):
        forward(1, c)
    for c in range(CHUNKS):
        arrived(1, c)
        rows = slice(c * rows_c, (c + 1) * rows_c)
        full_ref[rows, :] = hbuf[1, rows, :]
    if last:
        own_ref[...] = jnp.zeros_like(own_ref)
    for s in range(2):
        for c in range(CHUNKS):
            for k in range(4):
                pair_copy(s, c, k).wait_send()
                gather_copy(s, c, k).wait_send()
                if k < 3:
                    cross_copy(s, c, k).wait_send()
                    forward_copy(s, c, k).wait_send()


def mlp_block(layer, last, part, x, gains, biases, bout, bup, bdown, wup, wdown):
    batch, width = part.shape
    hidden = wup.shape[2]
    rows_o = batch // CHUNKS // 8
    any_spec = pl.BlockSpec(memory_space=pl.ANY)
    vmem_spec = pl.BlockSpec(memory_space=pltpu.VMEM)
    own = (CHUNKS, rows_o, width)
    own_shape = own if not last else (8, 128)
    dma = pltpu.SemaphoreType.DMA
    return pl.pallas_call(
        functools.partial(mlp_kernel, layer, last),
        out_shape=(jax.ShapeDtypeStruct((batch, width), BF16), jax.ShapeDtypeStruct(own_shape, BF16)),
        in_specs=[vmem_spec, any_spec if layer == 0 else vmem_spec] + [vmem_spec] * 5 + [any_spec] * 2,
        out_specs=(vmem_spec, vmem_spec),
        scratch_shapes=[
            pltpu.VMEM((width, hidden), BF16),
            pltpu.VMEM((hidden, width), BF16),
            pltpu.VMEM((batch, width), BF16),
            pltpu.VMEM((2, batch, width), BF16),
            pltpu.VMEM((batch // CHUNKS, hidden), BF16),
            pltpu.VMEM((2, CHUNKS, 4, rows_o, width), BF16),
            pltpu.VMEM((2, CHUNKS, 3, rows_o, width), BF16),
            pltpu.VMEM((2, CHUNKS, 3, rows_o, width), BF16),
            pltpu.VMEM(own, F32),
            pltpu.VMEM(own, BF16),
            dma((2 + CHUNKS,)),
            dma((2, CHUNKS, 4)),
            dma((2, CHUNKS, 4)),
            dma((2, CHUNKS, 3)),
            dma((2, CHUNKS, 3)),
            dma((2, CHUNKS, 4)),
            dma((2, CHUNKS, 4)),
            dma((2, CHUNKS, 3)),
            dma((2, CHUNKS, 3)),
        ],
        compiler_params=pltpu.CompilerParams(
            collective_id=layer, has_side_effects=True, vmem_limit_bytes=60 * 1024 * 1024),
        name=f"mlp_{layer}",
    )(part, x, gains, biases, bout, bup, bdown, wup, wdown)


def solution(mesh):
    cache_spec = P(None, 'dp', 'tp', None, None)
    in_specs = (P('dp', None), P('dp'), cache_spec, cache_spec, P(), P(),
                P(None, None, None, 'tp', None), P(None, None, 'tp', None),
                P(None, 'tp', None, None), P(), P(None, None, 'tp'), P(None, 'tp'),
                P(None, 'tp', None), P())
    out_specs = (P('dp', None), cache_spec, cache_spec)

    def local_step(x, cache_len, k_cache, v_cache, norm_gain, norm_bias, w_qkv, b_qkv, w_out, b_out, w_up, b_up, w_down, b_down):
        layers, batch, heads, slots, head = k_cache.shape
        width = x.shape[1]
        hd = heads * head
        k_in = jnp.swapaxes(k_cache, 3, 4).reshape(layers, batch, hd, slots)
        v_in = jnp.swapaxes(v_cache, 3, 4).reshape(layers, batch, hd, slots)
        wqkv = jnp.transpose(w_qkv, (0, 2, 3, 4, 1)).reshape(layers, 3 * hd, width)
        bqkv = b_qkv.reshape(layers, 3 * hd)
        wout = w_out.reshape(layers, hd, width)
        gains = norm_gain.reshape(2 * layers, width)
        biases = norm_bias.reshape(2 * layers, width)

        k_out = v_out = None
        rows, own = x, x
        for layer in range(layers):
            extra = () if layer == 0 else (k_out, v_out)
            k_out, v_out, part = attention(layer, cache_len, rows, gains, biases, bqkv, wqkv, wout, k_in, v_in, *extra)
            rows, own = mlp_block(layer, layer == layers - 1, part, own, gains, biases, b_out, b_up, b_down, w_up, w_down)

        def back(cache):
            return jnp.swapaxes(cache.reshape(layers, batch, heads, head, slots), 3, 4)

        return rows, back(k_out), back(v_out)

    return jax.shard_map(local_step, mesh=mesh, in_specs=in_specs, out_specs=out_specs, check_vma=False)
```

```python
import functools

import jax
import jax.numpy as jnp
from jax import lax
from jax.experimental import pallas as pl
from jax.experimental.pallas import tpu as pltpu
from jax.sharding import PartitionSpec as P

NORM_EPS = 1e-5
MESH = pl.DeviceIdType.MESH
F32 = jnp.float32
BF16 = jnp.bfloat16
NT = (((1,), (1,)), ((), ()))
NN = (((1,), (0,)), ((), ()))

GROUP = 16
RING = 3
PIECES = 8
CHUNKS = 2


def dot(lhs, rhs, dims=NN):
    return lax.dot_general(lhs, rhs, dims, preferred_element_type=F32)


def norm(rows, gain, bias):
    mean = jnp.mean(rows, axis=-1, keepdims=True)
    centered = rows - mean
    var = jnp.mean(centered * centered, axis=-1, keepdims=True)
    return centered * lax.rsqrt(var + NORM_EPS) * gain + bias


def attention_kernel(layer, in_place, lens, x_hbm, gain_ref, bias_ref, bqkv_ref, wqkv_hbm, wout_hbm, k_in, v_in, *rest):
    if layer > 0:
        rest = rest[2:]
    ko_hbm, vo_hbm, part_ref, kbuf, vbuf, xbuf, wqkv, wout, hbuf, kcols, vcols, qbuf, qrep, sbuf, abuf, w_sem, k_sem, v_sem, ko_sem, vo_sem = rest
    batch, width = xbuf.shape
    hd = wout.shape[0]
    head = hd // 4
    slots = kbuf.shape[2]
    groups = batch // GROUP
    n = GROUP * 4
    ring = kbuf.shape[0] // GROUP

    x_copy = pltpu.make_async_copy(x_hbm, xbuf, w_sem.at[0])
    x_copy.start()
    w_copy = pltpu.make_async_copy(wqkv_hbm.at[layer], wqkv, w_sem.at[1])
    w_copy.start()

    def load(src, buf, sem, g):
        rows = pl.ds(g * GROUP, GROUP)
        return pltpu.make_async_copy(src.at[layer, rows], buf.at[rows], sem.at[g])

    def save(buf, dst, sem, g):
        rows = pl.ds(g * GROUP, GROUP)
        here = rows if in_place else pl.ds(lax.rem(g, ring) * GROUP, GROUP)
        return pltpu.make_async_copy(buf.at[here], dst.at[layer, rows], sem.at[g])

    if in_place:
        def start_loads(g, carry):
            load(k_in, kbuf, k_sem, g).start()
            load(v_in, vbuf, v_sem, g).start()
            return carry

        lax.fori_loop(0, groups, start_loads, 0)
    o_copy = pltpu.make_async_copy(wout_hbm.at[layer], wout, w_sem.at[2])
    o_copy.start()

    spread_cols = (lax.broadcasted_iota(jnp.int32, (head, hd), 0) == lax.broadcasted_iota(jnp.int32, (head, hd), 1) % head).astype(F32).astype(BF16)
    head_of = lax.broadcasted_iota(jnp.int32, (4, hd), 0) == lax.broadcasted_iota(jnp.int32, (4, hd), 1) // head

    def bias_row(part):
        wide = dot(bqkv_ref[layer, part], spread_cols)
        return jnp.sum(jnp.where(head_of, wide, 0.0), axis=0, keepdims=True)

    bias_q = bias_row(0)
    bias_kv = [jnp.broadcast_to(bias_row(part), (128, hd)).T for part in (1, 2)]

    x_copy.wait()
    if layer == 0:
        gain = gain_ref[0, 0:1, :]
        bias = bias_ref[0, 0:1, :]

        def norm_rows(i, carry):
            rows = pl.ds(i * 32, 32)
            hbuf[rows, :] = norm(xbuf[rows, :].astype(F32), gain, bias).astype(BF16)
            return carry

        lax.fori_loop(0, batch // 32, norm_rows, 0)
    else:
        hbuf = xbuf
    w_copy.wait()
    for part, pages in ((1, kcols), (2, vcols)):
        for half in range(batch // 128):
            cols = dot(wqkv[part * hd:(part + 1) * hd, :], hbuf[half * 128:(half + 1) * 128, :], NT) + bias_kv[part - 1]
            cols = cols.astype(BF16).astype(F32)
            for j in range(128 // GROUP):
                pages[half * (128 // GROUP) + j] = cols if j == 0 else pltpu.roll(cols, 128 - j * GROUP, 1)
    qbuf[...] = (dot(hbuf[...], wqkv[0:hd, :], NT) + bias_q).astype(BF16)
    own_head = lax.broadcasted_iota(jnp.int32, (n, hd), 0) % 4 == lax.broadcasted_iota(jnp.int32, (n, hd), 1) // head
    repeat = (lax.broadcasted_iota(jnp.int32, (n, GROUP), 0) // 4 == lax.broadcasted_iota(jnp.int32, (n, GROUP), 1)).astype(F32).astype(BF16)
    for g in range(groups):
        qrep[g * n:(g + 1) * n, :] = jnp.where(own_head, dot(repeat, qbuf[g * GROUP:(g + 1) * GROUP, :]), 0.0).astype(BF16)

    lane8 = lax.broadcasted_iota(jnp.int32, (8, slots), 1)
    top8 = lax.broadcasted_iota(jnp.int32, (8, slots), 0) < 4
    lane_hd = lax.broadcasted_iota(jnp.int32, (hd, slots), 1)
    scale = head ** -0.5

    def updated(src, dst, cols, g, b):
        base = g * GROUP
        column = jnp.broadcast_to(cols[:, b:b + 1], (hd, slots)).astype(BF16)
        tile = jnp.where(lane_hd == lens[base + b], column, src[base + b])
        dst[base + b if in_place else lax.rem(g, ring) * GROUP + b] = tile
        return tile

    def key_stage(g):
        base = g * GROUP
        cols = kcols[g]
        q_rows = qrep[pl.ds(pl.multiple_of(base * 4, n), n), :]
        masked = []
        for i in range(0, GROUP, 2):
            tiles = [updated(kbuf if in_place else k_in, kbuf, cols, g, b) for b in (i, i + 1)]
            both = dot(q_rows[i * 4:i * 4 + 8, :], jnp.concatenate(tiles, axis=1))
            score = jnp.where(top8, both[:, 0:slots], both[:, slots:2 * slots]) * scale
            limit = jnp.where(top8, lens[base + i], lens[base + i + 1])
            masked.append(jnp.where(lane8 <= limit, score, -1e30))
        return jnp.concatenate(masked, axis=0)

    def value_stage(g, scores):
        weights = jnp.exp(scores - jnp.max(scores, axis=-1, keepdims=True))
        prob = weights / jnp.sum(weights, axis=-1, keepdims=True)
        cols = vcols[g]
        outs = []
        for i in range(0, GROUP, 2):
            tiles = [updated(vbuf if in_place else v_in, vbuf, cols, g, b) for b in (i, i + 1)]
            pair = prob[i * 4:i * 4 + 8, :]
            spread = jnp.concatenate([jnp.where(top8, pair, 0.0), jnp.where(top8, 0.0, pair)], axis=1).astype(BF16)
            outs.append(dot(spread, jnp.concatenate(tiles, axis=1), NT))
        heads = jnp.where(own_head, jnp.concatenate(outs, axis=0), 0.0).astype(BF16)
        abuf[pl.ds(pl.multiple_of(g * n, n), n), :] = heads

    def reuse(buf, dst, sem, g):
        if not in_place:
            @pl.when(g >= ring)
            def _():
                save(buf, dst, sem, g - ring).wait()

    if in_place:
        load(k_in, kbuf, k_sem, 0).wait()
    sbuf[0] = key_stage(0)
    save(kbuf, ko_hbm, ko_sem, 0).start()

    def step(g, carry):
        if in_place:
            load(v_in, vbuf, v_sem, g - 1).wait()
            load(k_in, kbuf, k_sem, g).wait()
        reuse(kbuf, ko_hbm, ko_sem, g)
        reuse(vbuf, vo_hbm, vo_sem, g - 1)
        scores = sbuf[lax.rem(g - 1, 2)]
        sbuf[lax.rem(g, 2)] = key_stage(g)
        value_stage(g - 1, scores)
        save(kbuf, ko_hbm, ko_sem, g).start()
        save(vbuf, vo_hbm, vo_sem, g - 1).start()
        return carry

    lax.fori_loop(1, groups, step, 0)
    final = groups - 1
    if in_place:
        load(v_in, vbuf, v_sem, final).wait()
    else:
        save(vbuf, vo_hbm, vo_sem, final - ring).wait()
    value_stage(final, sbuf[final % 2])
    save(vbuf, vo_hbm, vo_sem, final).start()
    o_copy.wait()
    collect = (lax.broadcasted_iota(jnp.int32, (GROUP, n), 1) // 4 == lax.broadcasted_iota(jnp.int32, (GROUP, n), 0)).astype(F32).astype(BF16)
    for g in range(groups):
        qbuf[g * GROUP:(g + 1) * GROUP, :] = dot(collect, abuf[g * n:(g + 1) * n, :]).astype(BF16)
    for c in range(0, width, 512):
        part_ref[:, c:c + 512] = dot(qbuf[...], wout[:, c:c + 512]).astype(BF16)

    def finish(g, carry):
        save(kbuf, ko_hbm, ko_sem, g).wait()
        save(vbuf, vo_hbm, vo_sem, g).wait()
        return carry

    lax.fori_loop(0 if in_place else groups - ring, groups, finish, 0)


def attention(layer, in_place, lens, x, gains, biases, bqkv, wqkv, wout, k_in, v_in, k_out=None, v_out=None):
    batch, width = x.shape
    hd, slots = k_in.shape[-2:]
    groups = batch // GROUP
    any_spec = pl.BlockSpec(memory_space=pl.ANY)
    vmem_spec = pl.BlockSpec(memory_space=pltpu.VMEM)
    cache_spec = any_spec if in_place else vmem_spec
    args = [lens, x, gains, biases, bqkv, wqkv, wout, k_in, v_in]
    specs = [pl.BlockSpec(memory_space=pltpu.SMEM), any_spec] + [vmem_spec] * 3 + [any_spec] * 2 + [cache_spec] * 2
    alias = {}
    shape = k_in.shape
    if layer > 0:
        args += [k_out, v_out]
        specs += [any_spec] * 2
        alias = {9: 0, 10: 1}
        shape = k_out.shape
    held = batch if in_place else RING * GROUP
    dma = pltpu.SemaphoreType.DMA
    return pl.pallas_call(
        functools.partial(attention_kernel, layer, in_place),
        out_shape=(
            jax.ShapeDtypeStruct(shape, BF16),
            jax.ShapeDtypeStruct(shape, BF16),
            jax.ShapeDtypeStruct((batch, width), BF16),
        ),
        in_specs=specs,
        out_specs=(any_spec, any_spec, vmem_spec),
        input_output_aliases=alias,
        scratch_shapes=[
            pltpu.VMEM((held, hd, slots), BF16),
            pltpu.VMEM((held, hd, slots), BF16),
            pltpu.VMEM((batch, width), BF16),
            pltpu.VMEM((3 * hd, width), BF16),
            pltpu.VMEM((hd, width), BF16),
            pltpu.VMEM((batch if layer == 0 else 16, width), BF16),
            pltpu.VMEM((groups, hd, 128), F32),
            pltpu.VMEM((groups, hd, 128), F32),
            pltpu.VMEM((batch, hd), BF16),
            pltpu.VMEM((batch * 4, hd), BF16),
            pltpu.VMEM((2, GROUP * 4, slots), F32),
            pltpu.VMEM((batch * 4, hd), BF16),
            dma((3,)),
            dma((groups,)),
            dma((groups,)),
            dma((groups,)),
            dma((groups,)),
        ],
        compiler_params=pltpu.CompilerParams(vmem_limit_bytes=(60 if in_place else 24) * 1024 * 1024),
        name=f"attention_{layer}",
    )(*args)


def mlp_kernel(layer, last, part_ref, x_ref, gain_ref, bias_ref, bout_ref, bup_ref, bdown_ref, wup_hbm, wdown_hbm, *rest):
    if last:
        full_ref, rest = rest[0], rest[1:]
    else:
        k_hbm, v_hbm, full_ref, own_ref, k_next, v_next = rest[:6]
        rest = rest[6:]
    (wup, wdown, part2, hbuf, ubuf, pair_in, cross_out, cross_in, own_sum, xown,
     w_sem, pair_s, pair_r, cross_s, cross_r, gat_s, gat_r, fwd_s, fwd_r, cache_sem) = rest
    batch, width = part_ref.shape
    hidden = wup.shape[1]
    rows_c = batch // CHUNKS
    rows_o = rows_c // 8
    me = lax.axis_index("tp")
    core = lax.rem(me, 2)
    chip = lax.div(me, 2)
    cx = lax.rem(chip, 2)
    cy = lax.div(chip, 2)
    partner = chip * 2 + 1 - core
    chips = ((1 - cy) * 2 + 1 - cx, cy * 2 + 1 - cx, (1 - cy) * 2 + cx, chip)

    def device(index):
        return {"tp": index}

    def rows_of(c, owner):
        return pl.ds(pl.multiple_of(c * rows_c + owner * rows_o, rows_o), rows_o)

    copies = [
        pltpu.make_async_copy(wup_hbm.at[layer], wup, w_sem.at[0]),
        pltpu.make_async_copy(wdown_hbm.at[layer], wdown, w_sem.at[1]),
    ]
    for copy in copies:
        copy.start()
    if layer == 0:
        x_copies = [pltpu.make_async_copy(x_ref.at[rows_of(c, me)], xown.at[c], w_sem.at[2 + c]) for c in range(CHUNKS)]
        for copy in x_copies:
            copy.start()

    caches = []
    if not last:
        piece = batch // PIECES
        for p in range(PIECES):
            rows = slice(p * piece, (p + 1) * piece)
            caches.append(pltpu.make_async_copy(k_hbm.at[layer + 1, rows], k_next.at[rows], cache_sem.at[0, p]))
            caches.append(pltpu.make_async_copy(v_hbm.at[layer + 1, rows], v_next.at[rows], cache_sem.at[1, p]))
        for copy in caches:
            copy.start()

    barrier = pltpu.get_barrier_semaphore()
    for peer in (partner,) + tuple(t * 2 + core for t in chips[:3]):
        pl.semaphore_signal(barrier, inc=1, device_id=device(peer), device_id_type=MESH)
    pl.semaphore_wait(barrier, 4)

    def remote(src, dst, send, recv, target):
        return pltpu.make_async_remote_copy(
            src_ref=src, dst_ref=dst, send_sem=send, recv_sem=recv, device_id=device(target), device_id_type=MESH)

    def pair_copy(s, c, k):
        src = part_ref if s == 0 else part2
        return remote(src.at[rows_of(c, chips[k] * 2 + 1 - core)], pair_in.at[s, c, k],
                      pair_s.at[s, c, k], pair_r.at[s, c, k], partner)

    def cross_copy(s, c, k):
        return remote(cross_out.at[s, c, k], cross_in.at[s, c, k],
                      cross_s.at[s, c, k], cross_r.at[s, c, k], chips[k] * 2 + core)

    def gather_copy(s, c, k):
        rows = rows_of(c, me)
        target = partner if k == 3 else chips[k] * 2 + core
        return remote(hbuf.at[s, rows], hbuf.at[s, rows], gat_s.at[s, c, k], gat_r.at[s, c, k], target)

    def forward_copy(s, c, k):
        rows = rows_of(c, chips[k] * 2 + core)
        return remote(hbuf.at[s, rows], hbuf.at[s, rows], fwd_s.at[s, c, k], fwd_r.at[s, c, k], partner)

    def send_pairs(s, c):
        for k in range(4):
            pair_copy(s, c, k).start()

    def add_pairs(s, c):
        src = part_ref if s == 0 else part2
        for k in range(4):
            pair_copy(s, c, k).wait_recv()
            both = src[rows_of(c, chips[k] * 2 + core), :].astype(F32) + pair_in[s, c, k].astype(F32)
            if k < 3:
                cross_out[s, c, k] = both.astype(BF16)
                cross_copy(s, c, k).start()
            else:
                own_sum[c] = both

    def own_total(s, c):
        total = own_sum[c]
        for k in (1, 2, 0):
            cross_copy(s, c, k).wait_recv()
            total = total + cross_in[s, c, k].astype(F32)
        return total

    def send_own(s, c):
        for k in range(4):
            gather_copy(s, c, k).start()

    def forward(s, c):
        for k in (1, 2, 0):
            gather_copy(s, c, k).wait_recv()
            forward_copy(s, c, k).start()

    def arrived(s, c):
        gather_copy(s, c, 3).wait_recv()
        for k in range(3):
            forward_copy(s, c, k).wait_recv()

    def row(ref, index):
        return ref[index:index + 1, :].astype(F32)

    def first_finish(c):
        total = own_total(0, c)
        old = xown[c] if layer == 0 else x_ref[c]
        mid = (old.astype(F32) + total + row(bout_ref, layer)).astype(BF16)
        xown[c] = mid
        hbuf[0, rows_of(c, me), :] = norm(mid.astype(F32), gain_ref[layer, 1:2, :], bias_ref[layer, 1:2, :]).astype(BF16)
        send_own(0, c)

    def second_finish(c):
        total = own_total(1, c)
        new = (xown[c].astype(F32) + total + row(bdown_ref, layer)).astype(BF16)
        if last:
            hbuf[1, rows_of(c, me), :] = new
        else:
            own_ref[c] = new
            hbuf[1, rows_of(c, me), :] = norm(new.astype(F32), gain_ref[layer + 1, 0:1, :], bias_ref[layer + 1, 0:1, :]).astype(BF16)
        send_own(1, c)

    def mlp(c):
        rows = slice(c * rows_c, (c + 1) * rows_c)
        h = hbuf[0, rows, :]
        for n in range(0, hidden, 256):
            up = dot(h, wup[:, n:n + 256]) + bup_ref[layer:layer + 1, n:n + 256].astype(F32)
            ubuf[:, n:n + 256] = jnp.maximum(up, 0.0).astype(BF16)
        u = ubuf[...]
        for n in range(0, width, 256):
            part2[rows, n:n + 256] = dot(u, wdown[:, n:n + 256]).astype(BF16)

    for c in range(CHUNKS):
        send_pairs(0, c)
    for c in range(CHUNKS):
        add_pairs(0, c)
    if layer == 0:
        for copy in x_copies:
            copy.wait()
    for c in range(CHUNKS):
        first_finish(c)
    for copy in copies:
        copy.wait()
    for c in range(CHUNKS):
        forward(0, c)
        if c > 0:
            add_pairs(1, c - 1)
        arrived(0, c)
        mlp(c)
        send_pairs(1, c)
    add_pairs(1, CHUNKS - 1)
    for c in range(CHUNKS):
        second_finish(c)
    for c in range(CHUNKS):
        forward(1, c)
    for c in range(CHUNKS):
        arrived(1, c)
        rows = slice(c * rows_c, (c + 1) * rows_c)
        full_ref[rows, :] = hbuf[1, rows, :]
    for copy in caches:
        copy.wait()
    for s in range(2):
        for c in range(CHUNKS):
            for k in range(4):
                pair_copy(s, c, k).wait_send()
                gather_copy(s, c, k).wait_send()
                if k < 3:
                    cross_copy(s, c, k).wait_send()
                    forward_copy(s, c, k).wait_send()


def mlp_block(layer, last, part, x, gains, biases, bout, bup, bdown, wup, wdown, k_in, v_in):
    batch, width = part.shape
    hidden = wup.shape[2]
    rows_o = batch // CHUNKS // 8
    any_spec = pl.BlockSpec(memory_space=pl.ANY)
    vmem_spec = pl.BlockSpec(memory_space=pltpu.VMEM)
    own = (CHUNKS, rows_o, width)
    args = [part, x, gains, biases, bout, bup, bdown, wup, wdown]
    in_specs = [vmem_spec, any_spec if layer == 0 else vmem_spec] + [vmem_spec] * 5 + [any_spec] * 2
    out_shape = [jax.ShapeDtypeStruct((batch, width), BF16)]
    if not last:
        args += [k_in, v_in]
        in_specs += [any_spec] * 2
        out_shape += [jax.ShapeDtypeStruct(own, BF16), pltpu.VMEM(k_in.shape[1:], BF16), pltpu.VMEM(v_in.shape[1:], BF16)]
    dma = pltpu.SemaphoreType.DMA
    return pl.pallas_call(
        functools.partial(mlp_kernel, layer, last),
        out_shape=out_shape,
        in_specs=in_specs,
        out_specs=[vmem_spec] * len(out_shape),
        scratch_shapes=[
            pltpu.VMEM((width, hidden), BF16),
            pltpu.VMEM((hidden, width), BF16),
            pltpu.VMEM((batch, width), BF16),
            pltpu.VMEM((2, batch, width), BF16),
            pltpu.VMEM((batch // CHUNKS, hidden), BF16),
            pltpu.VMEM((2, CHUNKS, 4, rows_o, width), BF16),
            pltpu.VMEM((2, CHUNKS, 3, rows_o, width), BF16),
            pltpu.VMEM((2, CHUNKS, 3, rows_o, width), BF16),
            pltpu.VMEM(own, F32),
            pltpu.VMEM(own, BF16),
            dma((2 + CHUNKS,)),
            dma((2, CHUNKS, 4)),
            dma((2, CHUNKS, 4)),
            dma((2, CHUNKS, 3)),
            dma((2, CHUNKS, 3)),
            dma((2, CHUNKS, 4)),
            dma((2, CHUNKS, 4)),
            dma((2, CHUNKS, 3)),
            dma((2, CHUNKS, 3)),
            dma((2, PIECES)),
        ],
        compiler_params=pltpu.CompilerParams(
            collective_id=layer, has_side_effects=True, vmem_limit_bytes=(60 if last else 24) * 1024 * 1024),
        name=f"mlp_{layer}",
    )(*args)


def solution(mesh):
    cache_spec = P(None, 'dp', 'tp', None, None)
    in_specs = (P('dp', None), P('dp'), cache_spec, cache_spec, P(), P(),
                P(None, None, None, 'tp', None), P(None, None, 'tp', None),
                P(None, 'tp', None, None), P(), P(None, None, 'tp'), P(None, 'tp'),
                P(None, 'tp', None), P())
    out_specs = (P('dp', None), cache_spec, cache_spec)

    def local_step(x, cache_len, k_cache, v_cache, norm_gain, norm_bias, w_qkv, b_qkv, w_out, b_out, w_up, b_up, w_down, b_down):
        layers, batch, heads, slots, head = k_cache.shape
        width = x.shape[1]
        hd = heads * head
        k_in = jnp.swapaxes(k_cache, 3, 4).reshape(layers, batch, hd, slots)
        v_in = jnp.swapaxes(v_cache, 3, 4).reshape(layers, batch, hd, slots)
        wqkv = jnp.transpose(w_qkv, (0, 2, 3, 4, 1)).reshape(layers, 3 * hd, width)
        wout = w_out.reshape(layers, hd, width)

        rows, own = x, x
        caches = (k_in, v_in)
        for layer in range(layers):
            k_out, v_out, part = attention(layer, layer == 0, cache_len, rows, norm_gain, norm_bias, b_qkv, wqkv, wout, *caches)
            last = layer == layers - 1
            rows, *held = mlp_block(layer, last, part, own, norm_gain, norm_bias, b_out, b_up, b_down, w_up, w_down, k_in, v_in)
            if not last:
                own, k_next, v_next = held
                caches = (pltpu.with_memory_space_constraint(k_next, pltpu.VMEM), pltpu.with_memory_space_constraint(v_next, pltpu.VMEM), k_out, v_out)

        def back(cache):
            return jnp.swapaxes(cache.reshape(layers, batch, heads, head, slots), 3, 4)

        return rows, back(k_out), back(v_out)

    return jax.shard_map(local_step, mesh=mesh, in_specs=in_specs, out_specs=out_specs, check_vma=False)
```

```python
import functools

import jax
import jax.numpy as jnp
from jax import lax
from jax.experimental import pallas as pl
from jax.experimental.pallas import tpu as pltpu
from jax.sharding import PartitionSpec as P

NORM_EPS = 1e-5
MESH = pl.DeviceIdType.MESH
F32 = jnp.float32
BF16 = jnp.bfloat16
NT = (((1,), (1,)), ((), ()))
NN = (((1,), (0,)), ((), ()))

GROUP = 16
RING = 3
PIECES = 8
CHUNKS = 2


def dot(lhs, rhs, dims=NN):
    return lax.dot_general(lhs, rhs, dims, preferred_element_type=F32)


def norm(rows, gain, bias):
    mean = jnp.mean(rows, axis=-1, keepdims=True)
    centered = rows - mean
    var = jnp.mean(centered * centered, axis=-1, keepdims=True)
    return centered * lax.rsqrt(var + NORM_EPS) * gain + bias


def attention_kernel(layer, fetch, lens, x_hbm, gain_ref, bias_ref, bqkv_ref, wqkv_hbm, wout_hbm, k_in, v_in, *rest):
    if layer > 0:
        rest = rest[2:]
    if fetch:
        k_hbm, v_hbm = k_in, v_in
        k_in, v_in = rest[-2:]
        rest = rest[:-2]
    ko_hbm, vo_hbm, part_ref, kbuf, vbuf, xbuf, wqkv, wout, hbuf, kcols, vcols, qbuf, qrep, sbuf, abuf, w_sem, k_sem, v_sem, ko_sem, vo_sem = rest
    batch, width = x_hbm.shape
    hd = wout.shape[0]
    head = hd // 4
    slots = kbuf.shape[2]
    groups = batch // GROUP
    n = GROUP * 4
    ring = kbuf.shape[0] // GROUP

    x_copy = pltpu.make_async_copy(x_hbm, xbuf, w_sem.at[0])
    x_copy.start()
    w_copy = pltpu.make_async_copy(wqkv_hbm.at[layer], wqkv, w_sem.at[1])
    w_copy.start()

    def load(src, buf, sem, g):
        rows = pl.ds(g * GROUP, GROUP)
        return pltpu.make_async_copy(src.at[layer, rows], buf.at[rows], sem.at[g])

    def save(buf, dst, sem, g):
        rows = pl.ds(g * GROUP, GROUP)
        here = pl.ds(lax.rem(g, ring) * GROUP, GROUP)
        return pltpu.make_async_copy(buf.at[here], dst.at[layer, rows], sem.at[g])

    if fetch:
        def start_loads(g, carry):
            load(k_hbm, k_in, k_sem, g).start()
            load(v_hbm, v_in, v_sem, g).start()
            return carry

        lax.fori_loop(0, groups, start_loads, 0)
    o_copy = pltpu.make_async_copy(wout_hbm.at[layer], wout, w_sem.at[2])
    o_copy.start()

    spread_cols = (lax.broadcasted_iota(jnp.int32, (head, hd), 0) == lax.broadcasted_iota(jnp.int32, (head, hd), 1) % head).astype(F32).astype(BF16)
    head_of = lax.broadcasted_iota(jnp.int32, (4, hd), 0) == lax.broadcasted_iota(jnp.int32, (4, hd), 1) // head

    def bias_row(part):
        wide = dot(bqkv_ref[layer, part], spread_cols)
        return jnp.sum(jnp.where(head_of, wide, 0.0), axis=0, keepdims=True)

    bias_q = bias_row(0)
    bias_kv = [jnp.broadcast_to(bias_row(part), (128, hd)).T for part in (1, 2)]

    x_copy.wait()
    if layer == 0:
        gain = gain_ref[0, 0:1, :]
        bias = bias_ref[0, 0:1, :]

        def norm_rows(i, carry):
            rows = pl.ds(i * 32, 32)
            hbuf[rows, :] = norm(xbuf[rows, :].astype(F32), gain, bias).astype(BF16)
            return carry

        lax.fori_loop(0, batch // 32, norm_rows, 0)
    else:
        hbuf = xbuf
    w_copy.wait()
    for part, pages in ((1, kcols), (2, vcols)):
        for half in range(batch // 128):
            cols = dot(wqkv[part * hd:(part + 1) * hd, :], hbuf[half * 128:(half + 1) * 128, :], NT)
            pages[half] = (cols + bias_kv[part - 1]).astype(BF16)
    qbuf[...] = (dot(hbuf[...], wqkv[0:hd, :], NT) + bias_q).astype(BF16)
    own_head = lax.broadcasted_iota(jnp.int32, (n, hd), 0) % 4 == lax.broadcasted_iota(jnp.int32, (n, hd), 1) // head
    repeat = (lax.broadcasted_iota(jnp.int32, (n, GROUP), 0) // 4 == lax.broadcasted_iota(jnp.int32, (n, GROUP), 1)).astype(F32).astype(BF16)
    for g in range(groups):
        qrep[g * n:(g + 1) * n, :] = jnp.where(own_head, dot(repeat, qbuf[g * GROUP:(g + 1) * GROUP, :]), 0.0).astype(BF16)

    lane8 = lax.broadcasted_iota(jnp.int32, (8, slots), 1)
    top8 = lax.broadcasted_iota(jnp.int32, (8, slots), 0) < 4
    lane16 = lax.broadcasted_iota(jnp.int32, (16, slots), 1).astype(F32).astype(BF16)
    scale = head ** -0.5

    def updated(src, dst, cols, g, b):
        base = g * GROUP
        column = pltpu.roll(cols, (lens[base + b] - base - b) & (slots - 1), 1).reshape(hd // 16, 16, slots)
        here = lane16 == jnp.full((16, slots), lens[base + b].astype(F32), F32).astype(BF16)
        tile = jnp.where(here[None], column, src[base + b].reshape(hd // 16, 16, slots)).reshape(hd, slots)
        dst[lax.rem(g, ring) * GROUP + b] = tile
        return tile

    def key_pair(g, i, cols, q_rows):
        base = g * GROUP
        tiles = [updated(k_in, kbuf, cols, g, b) for b in (i, i + 1)]
        both = dot(q_rows[i * 4:i * 4 + 8, :], jnp.concatenate(tiles, axis=1))
        score = jnp.where(top8, both[:, 0:slots], both[:, slots:2 * slots]) * scale
        limit = jnp.where(top8, lens[base + i], lens[base + i + 1])
        return jnp.where(lane8 <= limit, score, -1e30)

    def value_pair(g, i, cols, prob):
        tiles = [updated(v_in, vbuf, cols, g, b) for b in (i, i + 1)]
        pair = prob[i * 4:i * 4 + 8, :]
        spread = jnp.concatenate([jnp.where(top8, pair, 0.0), jnp.where(top8, 0.0, pair)], axis=1).astype(BF16)
        return dot(spread, jnp.concatenate(tiles, axis=1), NT)

    def stage(key_group, value_group):
        if value_group is not None:
            scores = sbuf[lax.rem(value_group, 2)]
            weights = jnp.exp(scores - jnp.max(scores, axis=-1, keepdims=True))
            prob = weights / jnp.sum(weights, axis=-1, keepdims=True)
            v_cols = vcols[lax.div(value_group, 128 // GROUP)]
        if key_group is not None:
            k_cols = kcols[lax.div(key_group, 128 // GROUP)]
            q_rows = qrep[pl.ds(pl.multiple_of(key_group * n, n), n), :]
        masked, outs = [], []
        for i in range(0, GROUP, 2):
            if key_group is not None:
                masked.append(key_pair(key_group, i, k_cols, q_rows))
            if value_group is not None:
                outs.append(value_pair(value_group, i, v_cols, prob))
        if key_group is not None:
            sbuf[lax.rem(key_group, 2)] = jnp.concatenate(masked, axis=0)
        if value_group is not None:
            heads = jnp.where(own_head, jnp.concatenate(outs, axis=0), 0.0).astype(BF16)
            abuf[pl.ds(pl.multiple_of(value_group * n, n), n), :] = heads

    def reuse(buf, dst, sem, g):
        @pl.when(g >= ring)
        def _():
            save(buf, dst, sem, g - ring).wait()

    if fetch:
        load(k_hbm, k_in, k_sem, 0).wait()
    stage(jnp.int32(0), None)
    save(kbuf, ko_hbm, ko_sem, 0).start()

    def step(g, carry):
        if fetch:
            load(v_hbm, v_in, v_sem, g - 1).wait()
            load(k_hbm, k_in, k_sem, g).wait()
        reuse(kbuf, ko_hbm, ko_sem, g)
        reuse(vbuf, vo_hbm, vo_sem, g - 1)
        stage(g, g - 1)
        save(kbuf, ko_hbm, ko_sem, g).start()
        save(vbuf, vo_hbm, vo_sem, g - 1).start()
        return carry

    lax.fori_loop(1, groups, step, 0)
    final = groups - 1
    if fetch:
        load(v_hbm, v_in, v_sem, final).wait()
    save(vbuf, vo_hbm, vo_sem, final - ring).wait()
    stage(None, jnp.int32(final))
    save(vbuf, vo_hbm, vo_sem, final).start()
    o_copy.wait()
    collect = (lax.broadcasted_iota(jnp.int32, (GROUP, n), 1) // 4 == lax.broadcasted_iota(jnp.int32, (GROUP, n), 0)).astype(F32).astype(BF16)
    for g in range(groups):
        qbuf[g * GROUP:(g + 1) * GROUP, :] = dot(collect, abuf[g * n:(g + 1) * n, :]).astype(BF16)
    for c in range(0, width, 512):
        part_ref[:, c:c + 512] = dot(qbuf[...], wout[:, c:c + 512]).astype(BF16)

    def finish(g, carry):
        save(kbuf, ko_hbm, ko_sem, g).wait()
        save(vbuf, vo_hbm, vo_sem, g).wait()
        return carry

    lax.fori_loop(groups - ring, groups, finish, 0)


def attention(layer, fetch, lens, x, gains, biases, bqkv, wqkv, wout, k_in, v_in, k_out=None, v_out=None):
    batch, width = x.shape
    hd, slots = k_in.shape[-2:]
    groups = batch // GROUP
    any_spec = pl.BlockSpec(memory_space=pl.ANY)
    vmem_spec = pl.BlockSpec(memory_space=pltpu.VMEM)
    cache_spec = any_spec if fetch else vmem_spec
    args = [lens, x, gains, biases, bqkv, wqkv, wout, k_in, v_in]
    specs = [pl.BlockSpec(memory_space=pltpu.SMEM), any_spec] + [vmem_spec] * 3 + [any_spec] * 2 + [cache_spec] * 2
    alias = {}
    shape = k_in.shape
    if layer > 0:
        args += [k_out, v_out]
        specs += [any_spec] * 2
        alias = {9: 0, 10: 1}
        shape = k_out.shape
    held = RING * GROUP
    fetched = [pltpu.VMEM((batch, hd, slots), BF16)] * 2 if fetch else []
    dma = pltpu.SemaphoreType.DMA
    return pl.pallas_call(
        functools.partial(attention_kernel, layer, fetch),
        out_shape=(
            jax.ShapeDtypeStruct(shape, BF16),
            jax.ShapeDtypeStruct(shape, BF16),
            jax.ShapeDtypeStruct((batch, width), BF16),
        ),
        in_specs=specs,
        out_specs=(any_spec, any_spec, vmem_spec),
        input_output_aliases=alias,
        scratch_shapes=[
            pltpu.VMEM((held, hd, slots), BF16),
            pltpu.VMEM((held, hd, slots), BF16),
            pltpu.VMEM((batch, width), BF16),
            pltpu.VMEM((3 * hd, width), BF16),
            pltpu.VMEM((hd, width), BF16),
            pltpu.VMEM((batch if layer == 0 else 16, width), BF16),
            pltpu.VMEM((batch // 128, hd, 128), BF16),
            pltpu.VMEM((batch // 128, hd, 128), BF16),
            pltpu.VMEM((batch, hd), BF16),
            pltpu.VMEM((batch * 4, hd), BF16),
            pltpu.VMEM((2, GROUP * 4, slots), F32),
            pltpu.VMEM((batch * 4, hd), BF16),
            dma((3,)),
            dma((groups,)),
            dma((groups,)),
            dma((groups,)),
            dma((groups,)),
        ] + fetched,
        compiler_params=pltpu.CompilerParams(vmem_limit_bytes=(60 if fetch else 24) * 1024 * 1024),
        name=f"attention_{layer}",
    )(*args)


def in_vmem(array):
    return pltpu.with_memory_space_constraint(array, pltpu.VMEM)


def mlp_kernel(layer, last, part_ref, x_ref, gain_ref, bias_ref, bout_ref, bup_ref, bdown_ref, wup_hbm, wdown_hbm, *rest):
    if last:
        full_ref, rest = rest[0], rest[1:]
    else:
        k_hbm, v_hbm, full_ref, own_ref, k_next, v_next = rest[:6]
        rest = rest[6:]
    (wup, wdown, part2, hbuf, ubuf, pair_in, cross_out, cross_in, own_sum, xown,
     w_sem, pair_s, pair_r, cross_s, cross_r, gat_s, gat_r, fwd_s, fwd_r, cache_sem) = rest
    batch, width = part_ref.shape
    hidden = wup.shape[1]
    rows_c = batch // CHUNKS
    rows_o = rows_c // 8
    me = lax.axis_index("tp")
    core = lax.rem(me, 2)
    chip = lax.div(me, 2)
    cx = lax.rem(chip, 2)
    cy = lax.div(chip, 2)
    partner = chip * 2 + 1 - core
    chips = ((1 - cy) * 2 + 1 - cx, cy * 2 + 1 - cx, (1 - cy) * 2 + cx, chip)

    def device(index):
        return {"tp": index}

    def rows_of(c, owner):
        return pl.ds(pl.multiple_of(c * rows_c + owner * rows_o, rows_o), rows_o)

    barrier = pltpu.get_barrier_semaphore()
    for peer in (partner,) + tuple(t * 2 + core for t in chips[:3]):
        pl.semaphore_signal(barrier, inc=1, device_id=device(peer), device_id_type=MESH)
    pl.semaphore_wait(barrier, 4)

    def remote(src, dst, send, recv, target):
        return pltpu.make_async_remote_copy(
            src_ref=src, dst_ref=dst, send_sem=send, recv_sem=recv, device_id=device(target), device_id_type=MESH)

    def pair_copy(s, c, k):
        src = part_ref if s == 0 else part2
        return remote(src.at[rows_of(c, chips[k] * 2 + 1 - core)], pair_in.at[s, c, k],
                      pair_s.at[s, c, k], pair_r.at[s, c, k], partner)

    def cross_copy(s, c, k):
        return remote(cross_out.at[s, c, k], cross_in.at[s, c, k],
                      cross_s.at[s, c, k], cross_r.at[s, c, k], chips[k] * 2 + core)

    def gather_copy(s, c, k):
        rows = rows_of(c, me)
        target = partner if k == 3 else chips[k] * 2 + core
        return remote(hbuf.at[s, rows], hbuf.at[s, rows], gat_s.at[s, c, k], gat_r.at[s, c, k], target)

    def forward_copy(s, c, k):
        rows = rows_of(c, chips[k] * 2 + core)
        return remote(hbuf.at[s, rows], hbuf.at[s, rows], fwd_s.at[s, c, k], fwd_r.at[s, c, k], partner)

    def send_pairs(s, c):
        for k in range(4):
            pair_copy(s, c, k).start()

    def add_pairs(s, c):
        src = part_ref if s == 0 else part2
        for k in range(4):
            pair_copy(s, c, k).wait_recv()
            both = src[rows_of(c, chips[k] * 2 + core), :].astype(F32) + pair_in[s, c, k].astype(F32)
            if k < 3:
                cross_out[s, c, k] = both.astype(BF16)
                cross_copy(s, c, k).start()
            else:
                own_sum[c] = both

    def own_total(s, c):
        total = own_sum[c]
        for k in (1, 2, 0):
            cross_copy(s, c, k).wait_recv()
            total = total + cross_in[s, c, k].astype(F32)
        return total

    def send_own(s, c):
        for k in range(4):
            gather_copy(s, c, k).start()

    def forward(s, c):
        for k in (1, 2, 0):
            gather_copy(s, c, k).wait_recv()
            forward_copy(s, c, k).start()

    def arrived(s, c):
        gather_copy(s, c, 3).wait_recv()
        for k in range(3):
            forward_copy(s, c, k).wait_recv()

    def row(ref, index):
        return ref[index:index + 1, :].astype(F32)

    def first_finish(c):
        total = own_total(0, c)
        old = xown[c] if layer == 0 else x_ref[c]
        mid = (old.astype(F32) + total + row(bout_ref, layer)).astype(BF16)
        xown[c] = mid
        hbuf[0, rows_of(c, me), :] = norm(mid.astype(F32), gain_ref[layer, 1:2, :], bias_ref[layer, 1:2, :]).astype(BF16)
        send_own(0, c)

    def second_finish(c):
        total = own_total(1, c)
        new = (xown[c].astype(F32) + total + row(bdown_ref, layer)).astype(BF16)
        if last:
            hbuf[1, rows_of(c, me), :] = new
        else:
            own_ref[c] = new
            hbuf[1, rows_of(c, me), :] = norm(new.astype(F32), gain_ref[layer + 1, 0:1, :], bias_ref[layer + 1, 0:1, :]).astype(BF16)
        send_own(1, c)

    def mlp(c):
        rows = slice(c * rows_c, (c + 1) * rows_c)
        h = hbuf[0, rows, :]
        for n in range(0, hidden, 256):
            up = dot(h, wup[:, n:n + 256]) + bup_ref[layer:layer + 1, n:n + 256].astype(F32)
            ubuf[:, n:n + 256] = jnp.maximum(up, 0.0).astype(BF16)
        u = ubuf[...]
        for n in range(0, width, 256):
            part2[rows, n:n + 256] = dot(u, wdown[:, n:n + 256]).astype(BF16)

    for c in range(CHUNKS):
        send_pairs(0, c)
    copies = [
        pltpu.make_async_copy(wup_hbm.at[layer], wup, w_sem.at[0]),
        pltpu.make_async_copy(wdown_hbm.at[layer], wdown, w_sem.at[1]),
    ]
    for copy in copies:
        copy.start()
    if layer == 0:
        x_copies = [pltpu.make_async_copy(x_ref.at[rows_of(c, me)], xown.at[c], w_sem.at[2 + c]) for c in range(CHUNKS)]
        for copy in x_copies:
            copy.start()

    caches = []
    if not last:
        piece = batch // PIECES
        for p in range(PIECES):
            rows = slice(p * piece, (p + 1) * piece)
            caches.append(pltpu.make_async_copy(k_hbm.at[layer + 1, rows], k_next.at[rows], cache_sem.at[0, p]))
            caches.append(pltpu.make_async_copy(v_hbm.at[layer + 1, rows], v_next.at[rows], cache_sem.at[1, p]))
    started = []

    def start_caches(count):
        for copy in caches[len(started):len(started) + count]:
            copy.start()
            started.append(copy)

    for c in range(CHUNKS):
        add_pairs(0, c)
        start_caches(2)
    if layer == 0:
        for copy in x_copies:
            copy.wait()
    for c in range(CHUNKS):
        first_finish(c)
        start_caches(2)
    for copy in copies:
        copy.wait()
    for c in range(CHUNKS):
        forward(0, c)
        if c > 0:
            add_pairs(1, c - 1)
        arrived(0, c)
        mlp(c)
        send_pairs(1, c)
        start_caches(2)
    add_pairs(1, CHUNKS - 1)
    start_caches(2)
    for c in range(CHUNKS):
        second_finish(c)
        start_caches(2 if c == 0 else 2 * PIECES)
    for c in range(CHUNKS):
        forward(1, c)
    for c in range(CHUNKS):
        arrived(1, c)
        rows = slice(c * rows_c, (c + 1) * rows_c)
        full_ref[rows, :] = hbuf[1, rows, :]
    for copy in caches:
        copy.wait()
    for s in range(2):
        for c in range(CHUNKS):
            for k in range(4):
                pair_copy(s, c, k).wait_send()
                gather_copy(s, c, k).wait_send()
                if k < 3:
                    cross_copy(s, c, k).wait_send()
                    forward_copy(s, c, k).wait_send()


def mlp_block(layer, last, part, x, gains, biases, bout, bup, bdown, wup, wdown, k_in, v_in):
    batch, width = part.shape
    hidden = wup.shape[2]
    rows_o = batch // CHUNKS // 8
    any_spec = pl.BlockSpec(memory_space=pl.ANY)
    vmem_spec = pl.BlockSpec(memory_space=pltpu.VMEM)
    own = (CHUNKS, rows_o, width)
    args = [part, x, gains, biases, bout, bup, bdown, wup, wdown]
    in_specs = [vmem_spec, any_spec if layer == 0 else vmem_spec] + [vmem_spec] * 5 + [any_spec] * 2
    out_shape = [jax.ShapeDtypeStruct((batch, width), BF16)]
    if not last:
        args += [k_in, v_in]
        in_specs += [any_spec] * 2
        out_shape += [jax.ShapeDtypeStruct(own, BF16), pltpu.VMEM(k_in.shape[1:], BF16), pltpu.VMEM(v_in.shape[1:], BF16)]
    dma = pltpu.SemaphoreType.DMA
    return pl.pallas_call(
        functools.partial(mlp_kernel, layer, last),
        out_shape=out_shape,
        in_specs=in_specs,
        out_specs=[vmem_spec] * len(out_shape),
        scratch_shapes=[
            pltpu.VMEM((width, hidden), BF16),
            pltpu.VMEM((hidden, width), BF16),
            pltpu.VMEM((batch, width), BF16),
            pltpu.VMEM((2, batch, width), BF16),
            pltpu.VMEM((batch // CHUNKS, hidden), BF16),
            pltpu.VMEM((2, CHUNKS, 4, rows_o, width), BF16),
            pltpu.VMEM((2, CHUNKS, 3, rows_o, width), BF16),
            pltpu.VMEM((2, CHUNKS, 3, rows_o, width), BF16),
            pltpu.VMEM(own, F32),
            pltpu.VMEM(own, BF16),
            dma((2 + CHUNKS,)),
            dma((2, CHUNKS, 4)),
            dma((2, CHUNKS, 4)),
            dma((2, CHUNKS, 3)),
            dma((2, CHUNKS, 3)),
            dma((2, CHUNKS, 4)),
            dma((2, CHUNKS, 4)),
            dma((2, CHUNKS, 3)),
            dma((2, CHUNKS, 3)),
            dma((2, PIECES)),
        ],
        compiler_params=pltpu.CompilerParams(
            collective_id=layer, has_side_effects=True, vmem_limit_bytes=(60 if last else 24) * 1024 * 1024),
        name=f"mlp_{layer}",
    )(*args)


def solution(mesh):
    cache_spec = P(None, 'dp', 'tp', None, None)
    in_specs = (P('dp', None), P('dp'), cache_spec, cache_spec, P(), P(),
                P(None, None, None, 'tp', None), P(None, None, 'tp', None),
                P(None, 'tp', None, None), P(), P(None, None, 'tp'), P(None, 'tp'),
                P(None, 'tp', None), P())
    out_specs = (P('dp', None), cache_spec, cache_spec)

    def local_step(x, cache_len, k_cache, v_cache, norm_gain, norm_bias, w_qkv, b_qkv, w_out, b_out, w_up, b_up, w_down, b_down):
        layers, batch, heads, slots, head = k_cache.shape
        width = x.shape[1]
        hd = heads * head
        k_in = jnp.swapaxes(k_cache, 3, 4).reshape(layers, batch, hd, slots)
        v_in = jnp.swapaxes(v_cache, 3, 4).reshape(layers, batch, hd, slots)
        wqkv = jnp.transpose(w_qkv, (0, 2, 3, 4, 1)).reshape(layers, 3 * hd, width)
        wout = w_out.reshape(layers, hd, width)

        rows, own = x, x
        caches = (k_in, v_in)
        for layer in range(layers):
            k_out, v_out, part = attention(layer, layer == 0, cache_len, rows, norm_gain, norm_bias, b_qkv, wqkv, wout, *caches)
            last = layer == layers - 1
            rows, *held = mlp_block(layer, last, part, own, norm_gain, norm_bias, b_out, b_up, b_down, w_up, w_down, k_in, v_in)
            if not last:
                own, k_next, v_next = held
                caches = (in_vmem(k_next), in_vmem(v_next), k_out, v_out)

        def back(cache):
            return jnp.swapaxes(cache.reshape(layers, batch, heads, head, slots), 3, 4)

        return rows, back(k_out), back(v_out)

    return jax.shard_map(local_step, mesh=mesh, in_specs=in_specs, out_specs=out_specs, check_vma=False)
```

```python
import functools

import jax
import jax.numpy as jnp
from jax import lax
from jax.experimental import pallas as pl
from jax.experimental.pallas import tpu as pltpu
from jax.sharding import PartitionSpec as P

NORM_EPS = 1e-5
MESH = pl.DeviceIdType.MESH
F32 = jnp.float32
BF16 = jnp.bfloat16
NT = (((1,), (1,)), ((), ()))
NN = (((1,), (0,)), ((), ()))

GROUP = 16
RING = 3
PIECES = 8
UPDATES = (4, 1, 1, 2, 3, 3, 2)
CHUNKS = 2


def dot(lhs, rhs, dims=NN):
    return lax.dot_general(lhs, rhs, dims, preferred_element_type=F32)


def norm(rows, gain, bias):
    mean = jnp.mean(rows, axis=-1, keepdims=True)
    centered = rows - mean
    var = jnp.mean(centered * centered, axis=-1, keepdims=True)
    return centered * lax.rsqrt(var + NORM_EPS) * gain + bias


def attention_kernel(layer, fetch, lens, x_hbm, gain_ref, bias_ref, bqkv_ref, wqkv_hbm, wout_hbm, k_in, v_in, *rest):
    if layer > 0:
        rest = rest[2:]
    if fetch:
        k_hbm, v_hbm = k_in, v_in
        k_in, v_in = rest[-2:]
        rest = rest[:-2]
    ko_hbm, vo_hbm, part_ref, kbuf, vbuf, xbuf, wqkv, wout, hbuf, kcols, vcols, qbuf, qrep, sbuf, abuf, w_sem, k_sem, v_sem, ko_sem, vo_sem = rest
    batch, width = x_hbm.shape
    hd = wout.shape[0]
    head = hd // 4
    slots = kbuf.shape[2]
    groups = batch // GROUP
    n = GROUP * 4
    ring = kbuf.shape[0] // GROUP

    x_copy = pltpu.make_async_copy(x_hbm, xbuf, w_sem.at[0])
    x_copy.start()
    w_copy = pltpu.make_async_copy(wqkv_hbm.at[layer], wqkv, w_sem.at[1])
    w_copy.start()

    def load(src, buf, sem, g):
        rows = pl.ds(g * GROUP, GROUP)
        return pltpu.make_async_copy(src.at[layer, rows], buf.at[rows], sem.at[g])

    def save(buf, dst, sem, g):
        rows = pl.ds(g * GROUP, GROUP)
        here = pl.ds(lax.rem(g, ring) * GROUP, GROUP)
        return pltpu.make_async_copy(buf.at[here], dst.at[layer, rows], sem.at[g])

    if fetch:
        def start_loads(g, carry):
            load(k_hbm, k_in, k_sem, g).start()
            load(v_hbm, v_in, v_sem, g).start()
            return carry

        lax.fori_loop(0, groups, start_loads, 0)
    o_copy = pltpu.make_async_copy(wout_hbm.at[layer], wout, w_sem.at[2])
    o_copy.start()

    spread_cols = (lax.broadcasted_iota(jnp.int32, (head, hd), 0) == lax.broadcasted_iota(jnp.int32, (head, hd), 1) % head).astype(F32).astype(BF16)
    head_of = lax.broadcasted_iota(jnp.int32, (4, hd), 0) == lax.broadcasted_iota(jnp.int32, (4, hd), 1) // head

    def bias_row(part):
        wide = dot(bqkv_ref[layer, part], spread_cols)
        return jnp.sum(jnp.where(head_of, wide, 0.0), axis=0, keepdims=True)

    bias_q = bias_row(0)
    bias_kv = [jnp.broadcast_to(bias_row(part), (128, hd)).T for part in (1, 2)]

    x_copy.wait()
    if layer == 0:
        gain = gain_ref[0, 0:1, :]
        bias = bias_ref[0, 0:1, :]

        def norm_rows(i, carry):
            rows = pl.ds(i * 32, 32)
            hbuf[rows, :] = norm(xbuf[rows, :].astype(F32), gain, bias).astype(BF16)
            return carry

        lax.fori_loop(0, batch // 32, norm_rows, 0)
    else:
        hbuf = xbuf
    w_copy.wait()
    for part, pages in ((1, kcols), (2, vcols)):
        for half in range(batch // 128):
            cols = dot(wqkv[part * hd:(part + 1) * hd, :], hbuf[half * 128:(half + 1) * 128, :], NT)
            pages[half] = (cols + bias_kv[part - 1]).astype(BF16)
    qbuf[...] = (dot(hbuf[...], wqkv[0:hd, :], NT) + bias_q).astype(BF16)
    own_head = lax.broadcasted_iota(jnp.int32, (n, hd), 0) % 4 == lax.broadcasted_iota(jnp.int32, (n, hd), 1) // head
    repeat = (lax.broadcasted_iota(jnp.int32, (n, GROUP), 0) // 4 == lax.broadcasted_iota(jnp.int32, (n, GROUP), 1)).astype(F32).astype(BF16)
    for g in range(groups):
        qrep[g * n:(g + 1) * n, :] = jnp.where(own_head, dot(repeat, qbuf[g * GROUP:(g + 1) * GROUP, :]), 0.0).astype(BF16)

    lane8 = lax.broadcasted_iota(jnp.int32, (8, slots), 1)
    top8 = lax.broadcasted_iota(jnp.int32, (8, slots), 0) < 4
    lane16 = lax.broadcasted_iota(jnp.int32, (16, slots), 1).astype(F32).astype(BF16)
    scale = head ** -0.5

    def updated(src, dst, cols, g, b):
        base = g * GROUP
        column = pltpu.roll(cols, (lens[base + b] - base - b) & (slots - 1), 1).reshape(hd // 16, 16, slots)
        here = lane16 == jnp.full((16, slots), lens[base + b].astype(F32), F32).astype(BF16)
        tile = jnp.where(here[None], column, src[base + b].reshape(hd // 16, 16, slots)).reshape(hd, slots)
        dst[lax.rem(g, ring) * GROUP + b] = tile
        return tile

    def key_pair(g, i, cols, q_rows):
        base = g * GROUP
        tiles = [updated(k_in, kbuf, cols, g, b) for b in (i, i + 1)]
        both = dot(q_rows[i * 4:i * 4 + 8, :], jnp.concatenate(tiles, axis=1))
        score = jnp.where(top8, both[:, 0:slots], both[:, slots:2 * slots]) * scale
        limit = jnp.where(top8, lens[base + i], lens[base + i + 1])
        return jnp.where(lane8 <= limit, score, -1e30)

    def value_pair(g, i, cols, prob):
        tiles = [updated(v_in, vbuf, cols, g, b) for b in (i, i + 1)]
        pair = prob[i * 4:i * 4 + 8, :]
        spread = jnp.concatenate([jnp.where(top8, pair, 0.0), jnp.where(top8, 0.0, pair)], axis=1).astype(BF16)
        return dot(spread, jnp.concatenate(tiles, axis=1), NT)

    def stage(key_group, value_group):
        if value_group is not None:
            scores = sbuf[lax.rem(value_group, 2)]
            weights = jnp.exp(scores - jnp.max(scores, axis=-1, keepdims=True))
            prob = weights / jnp.sum(weights, axis=-1, keepdims=True)
            v_cols = vcols[lax.div(value_group, 128 // GROUP)]
        if key_group is not None:
            k_cols = kcols[lax.div(key_group, 128 // GROUP)]
            q_rows = qrep[pl.ds(pl.multiple_of(key_group * n, n), n), :]
        masked, outs = [], []
        for i in range(0, GROUP, 2):
            if key_group is not None:
                masked.append(key_pair(key_group, i, k_cols, q_rows))
            if value_group is not None:
                outs.append(value_pair(value_group, i, v_cols, prob))
        if key_group is not None:
            sbuf[lax.rem(key_group, 2)] = jnp.concatenate(masked, axis=0)
        if value_group is not None:
            heads = jnp.where(own_head, jnp.concatenate(outs, axis=0), 0.0).astype(BF16)
            abuf[pl.ds(pl.multiple_of(value_group * n, n), n), :] = heads

    def reuse(buf, dst, sem, g):
        @pl.when(g >= ring)
        def _():
            save(buf, dst, sem, g - ring).wait()

    if fetch:
        load(k_hbm, k_in, k_sem, 0).wait()
    stage(jnp.int32(0), None)
    save(kbuf, ko_hbm, ko_sem, 0).start()

    def step(g, carry):
        if fetch:
            load(v_hbm, v_in, v_sem, g - 1).wait()
            load(k_hbm, k_in, k_sem, g).wait()
        reuse(kbuf, ko_hbm, ko_sem, g)
        reuse(vbuf, vo_hbm, vo_sem, g - 1)
        stage(g, g - 1)
        save(kbuf, ko_hbm, ko_sem, g).start()
        save(vbuf, vo_hbm, vo_sem, g - 1).start()
        return carry

    lax.fori_loop(1, groups, step, 0)
    final = groups - 1
    if fetch:
        load(v_hbm, v_in, v_sem, final).wait()
    save(vbuf, vo_hbm, vo_sem, final - ring).wait()
    stage(None, jnp.int32(final))
    save(vbuf, vo_hbm, vo_sem, final).start()
    o_copy.wait()
    collect = (lax.broadcasted_iota(jnp.int32, (GROUP, n), 1) // 4 == lax.broadcasted_iota(jnp.int32, (GROUP, n), 0)).astype(F32).astype(BF16)
    for g in range(groups):
        qbuf[g * GROUP:(g + 1) * GROUP, :] = dot(collect, abuf[g * n:(g + 1) * n, :]).astype(BF16)
    for c in range(0, width, 512):
        part_ref[:, c:c + 512] = dot(qbuf[...], wout[:, c:c + 512]).astype(BF16)

    def finish(g, carry):
        save(kbuf, ko_hbm, ko_sem, g).wait()
        save(vbuf, vo_hbm, vo_sem, g).wait()
        return carry

    lax.fori_loop(groups - ring, groups, finish, 0)


def attention(layer, fetch, lens, x, gains, biases, bqkv, wqkv, wout, k_in, v_in, k_out=None, v_out=None):
    batch, width = x.shape
    hd, slots = k_in.shape[-2:]
    groups = batch // GROUP
    any_spec = pl.BlockSpec(memory_space=pl.ANY)
    vmem_spec = pl.BlockSpec(memory_space=pltpu.VMEM)
    cache_spec = any_spec if fetch else vmem_spec
    args = [lens, x, gains, biases, bqkv, wqkv, wout, k_in, v_in]
    specs = [pl.BlockSpec(memory_space=pltpu.SMEM), any_spec] + [vmem_spec] * 3 + [any_spec] * 2 + [cache_spec] * 2
    alias = {}
    shape = k_in.shape
    if layer > 0:
        args += [k_out, v_out]
        specs += [any_spec] * 2
        alias = {9: 0, 10: 1}
        shape = k_out.shape
    held = RING * GROUP
    fetched = [pltpu.VMEM((batch, hd, slots), BF16)] * 2 if fetch else []
    dma = pltpu.SemaphoreType.DMA
    return pl.pallas_call(
        functools.partial(attention_kernel, layer, fetch),
        out_shape=(
            jax.ShapeDtypeStruct(shape, BF16),
            jax.ShapeDtypeStruct(shape, BF16),
            jax.ShapeDtypeStruct((batch, width), BF16),
        ),
        in_specs=specs,
        out_specs=(any_spec, any_spec, vmem_spec),
        input_output_aliases=alias,
        scratch_shapes=[
            pltpu.VMEM((held, hd, slots), BF16),
            pltpu.VMEM((held, hd, slots), BF16),
            pltpu.VMEM((batch, width), BF16),
            pltpu.VMEM((3 * hd, width), BF16),
            pltpu.VMEM((hd, width), BF16),
            pltpu.VMEM((batch if layer == 0 else 16, width), BF16),
            pltpu.VMEM((batch // 128, hd, 128), BF16),
            pltpu.VMEM((batch // 128, hd, 128), BF16),
            pltpu.VMEM((batch, hd), BF16),
            pltpu.VMEM((batch * 4, hd), BF16),
            pltpu.VMEM((2, GROUP * 4, slots), F32),
            pltpu.VMEM((batch * 4, hd), BF16),
            dma((3,)),
            dma((groups,)),
            dma((groups,)),
            dma((groups,)),
            dma((groups,)),
        ] + fetched,
        compiler_params=pltpu.CompilerParams(vmem_limit_bytes=(60 if fetch else 24) * 1024 * 1024),
        name=f"attention_{layer}",
    )(*args)


def middle_kernel(lens, part_ref, x_hbm, gain_ref, bias_ref, bqkv_ref, bout_ref, bup_ref, bdown_ref,
                  wqkv_hbm, wout_hbm, wup_hbm, wdown_hbm, k_hbm, v_hbm,
                  full_ref, keys, values,
                  wqkv, wout, wup, wdown, parts, hbuf, ubuf, pair_in, cross_out, cross_in, own_sum, xown,
                  qrep, kcols, vcols, vrows, sbuf, abuf,
                  w_sem, cache_sem, pair_s, pair_r, cross_s, cross_r, gat_s, gat_r, fwd_s, fwd_r):
    batch, width = part_ref.shape
    hidden = wup.shape[1]
    hd = wout.shape[0]
    head = hd // 4
    slots = keys.shape[2]
    rows_c = batch // CHUNKS
    rows_o = rows_c // 8
    n = GROUP * 4
    groups_c = rows_c // GROUP
    scale = head ** -0.5
    me = lax.axis_index("tp")
    core = lax.rem(me, 2)
    chip = lax.div(me, 2)
    cx = lax.rem(chip, 2)
    cy = lax.div(chip, 2)
    partner = chip * 2 + 1 - core
    chips = ((1 - cy) * 2 + 1 - cx, cy * 2 + 1 - cx, (1 - cy) * 2 + cx, chip)

    def rows_of(c, owner):
        return pl.ds(pl.multiple_of(c * rows_c + owner * rows_o, rows_o), rows_o)

    def remote(src, dst, send, recv, target):
        return pltpu.make_async_remote_copy(
            src_ref=src, dst_ref=dst, send_sem=send, recv_sem=recv, device_id={"tp": target}, device_id_type=MESH)

    def source(s):
        return part_ref if s == 0 else parts.at[s - 1]

    def pair_copy(s, c, k):
        return remote(source(s).at[rows_of(c, chips[k] * 2 + 1 - core)], pair_in.at[s % 2, c, k],
                      pair_s.at[s, c, k], pair_r.at[s, c, k], partner)

    def cross_copy(s, c, k):
        return remote(cross_out.at[s % 2, c, k], cross_in.at[s % 2, c, k],
                      cross_s.at[s, c, k], cross_r.at[s, c, k], chips[k] * 2 + core)

    def gather_copy(s, c, k):
        rows = rows_of(c, me)
        target = partner if k == 3 else chips[k] * 2 + core
        return remote(hbuf.at[s, rows], hbuf.at[s, rows], gat_s.at[s, c, k], gat_r.at[s, c, k], target)

    def forward_copy(s, c, k):
        rows = rows_of(c, chips[k] * 2 + core)
        return remote(hbuf.at[s, rows], hbuf.at[s, rows], fwd_s.at[s, c, k], fwd_r.at[s, c, k], partner)

    def send_pairs(s, c):
        for k in range(4):
            pair_copy(s, c, k).start()

    def add_pairs(s, c):
        for k in range(4):
            pair_copy(s, c, k).wait_recv()
            both = source(s)[rows_of(c, chips[k] * 2 + core), :].astype(F32) + pair_in[s % 2, c, k].astype(F32)
            if k < 3:
                if s > 1:
                    cross_copy(s - 2, c, k).wait_send()
                cross_out[s % 2, c, k] = both.astype(BF16)
                cross_copy(s, c, k).start()
            else:
                own_sum[c] = both

    def row(ref, index):
        return ref[index:index + 1, :].astype(F32)

    def finish(s, c):
        layer = s // 2
        total = own_sum[c]
        for k in (1, 2, 0):
            cross_copy(s, c, k).wait_recv()
            total = total + cross_in[s % 2, c, k].astype(F32)
        add = row(bout_ref, layer) if s % 2 == 0 else row(bdown_ref, layer)
        new = (xown[c].astype(F32) + total + add).astype(BF16)
        if s < 3:
            xown[c] = new
            at = s + 1
            new = norm(new.astype(F32), gain_ref[at // 2, at % 2:at % 2 + 1, :], bias_ref[at // 2, at % 2:at % 2 + 1, :]).astype(BF16)
        hbuf[s, rows_of(c, me), :] = new
        for k in range(4):
            gather_copy(s, c, k).start()

    def forward(s, c):
        for k in (1, 2, 0):
            gather_copy(s, c, k).wait_recv()
            forward_copy(s, c, k).start()

    def arrived(s, c):
        gather_copy(s, c, 3).wait_recv()
        for k in range(3):
            forward_copy(s, c, k).wait_recv()

    def mlp(layer, c):
        s = 2 * layer
        rows = slice(c * rows_c, (c + 1) * rows_c)
        h = hbuf[s, rows, :]
        for i in range(0, hidden, 256):
            up = dot(h, wup[:, i:i + 256]) + bup_ref[layer:layer + 1, i:i + 256].astype(F32)
            ubuf[:, i:i + 256] = jnp.maximum(up, 0.0).astype(BF16)
        u = ubuf[...]
        for i in range(0, width, 256):
            parts[s, rows, i:i + 256] = dot(u, wdown[:, i:i + 256]).astype(BF16)

    spread_cols = (lax.broadcasted_iota(jnp.int32, (head, hd), 0) == lax.broadcasted_iota(jnp.int32, (head, hd), 1) % head).astype(F32).astype(BF16)
    head_of = lax.broadcasted_iota(jnp.int32, (4, hd), 0) == lax.broadcasted_iota(jnp.int32, (4, hd), 1) // head
    own_head = lax.broadcasted_iota(jnp.int32, (n, hd), 0) % 4 == lax.broadcasted_iota(jnp.int32, (n, hd), 1) // head
    repeat = (lax.broadcasted_iota(jnp.int32, (n, GROUP), 0) // 4 == lax.broadcasted_iota(jnp.int32, (n, GROUP), 1)).astype(F32).astype(BF16)
    collect = (lax.broadcasted_iota(jnp.int32, (GROUP, n), 1) // 4 == lax.broadcasted_iota(jnp.int32, (GROUP, n), 0)).astype(F32).astype(BF16)
    top8 = lax.broadcasted_iota(jnp.int32, (8, slots), 0) < 4
    lane = lax.broadcasted_iota(jnp.int32, (n, slots), 1)
    row_seq = lax.broadcasted_iota(jnp.int32, (n, slots), 0) // 4
    lane16 = lax.broadcasted_iota(jnp.int32, (16, slots), 1).astype(F32).astype(BF16)

    def bias_row(part):
        wide = dot(bqkv_ref[1, part], spread_cols)
        return jnp.sum(jnp.where(head_of, wide, 0.0), axis=0, keepdims=True)

    def project(c):
        rows = slice(c * rows_c, (c + 1) * rows_c)
        h = hbuf[1, rows, :]
        q = (dot(h, wqkv[0:hd, :], NT) + bias_row(0)).astype(BF16)
        for g in range(groups_c):
            at = (c * groups_c + g) * n
            qrep[at:at + n, :] = jnp.where(own_head, dot(repeat, q[g * GROUP:(g + 1) * GROUP, :]), 0.0).astype(BF16)
        for part, cols in ((1, kcols), (2, vcols)):
            column = jnp.broadcast_to(bias_row(part), (128, hd)).T
            new = (dot(wqkv[part * hd:(part + 1) * hd, :], h, NT) + column).astype(BF16)
            cols[c] = new
            if part == 2:
                vrows[rows, :] = new.astype(F32).T.astype(BF16)

    def lengths(g):
        base = g * GROUP
        return jnp.concatenate([jnp.where(top8, lens[base + i], lens[base + i + 1]) for i in range(0, GROUP, 2)], axis=0)

    def stage(c, key_group, value_group):
        if value_group is not None:
            scores = sbuf[lax.rem(value_group, 2)]
            weights = jnp.exp(scores - jnp.max(scores, axis=-1, keepdims=True))
            prob = (weights / jnp.sum(weights, axis=-1, keepdims=True)).astype(BF16).astype(F32)
            at_new = lane == lengths(value_group)
            prob_new = jnp.sum(jnp.where(at_new, prob, 0.0), axis=-1, keepdims=True)
            prob = jnp.where(at_new, 0.0, prob)
        if key_group is not None:
            q_rows = qrep[pl.ds(pl.multiple_of(key_group * n, n), n), :]
        raw, outs = [], []
        for i in range(0, GROUP, 2):
            if key_group is not None:
                tiles = [keys[key_group * GROUP + b] for b in (i, i + 1)]
                both = dot(q_rows[i * 4:i * 4 + 8, :], jnp.concatenate(tiles, axis=1))
                raw.append(jnp.where(top8, both[:, 0:slots], both[:, slots:2 * slots]))
            if value_group is not None:
                tiles = [values[value_group * GROUP + b] for b in (i, i + 1)]
                pair = prob[i * 4:i * 4 + 8, :]
                spread = jnp.concatenate([jnp.where(top8, pair, 0.0), jnp.where(top8, 0.0, pair)], axis=1).astype(BF16)
                outs.append(dot(spread, jnp.concatenate(tiles, axis=1), NT))
        if key_group is not None:
            cross = dot(q_rows, kcols[c])
            mine = lane == row_seq + (key_group - c * groups_c) * GROUP
            score_new = jnp.sum(jnp.where(mine, cross, 0.0), axis=-1, keepdims=True)
            limit = lengths(key_group)
            score = jnp.where(lane == limit, score_new, jnp.concatenate(raw, axis=0)) * scale
            sbuf[lax.rem(key_group, 2)] = jnp.where(lane <= limit, score, -1e30)
        if value_group is not None:
            v_rep = dot(repeat, vrows[pl.ds(pl.multiple_of(value_group * GROUP, GROUP), GROUP), :])
            heads = jnp.where(own_head, jnp.concatenate(outs, axis=0) + prob_new * v_rep, 0.0).astype(BF16)
            abuf[pl.ds(pl.multiple_of(value_group * GROUP, GROUP), GROUP), :] = dot(collect, heads).astype(BF16)

    def attend(c):
        first, end = c * groups_c, (c + 1) * groups_c
        stage(c, jnp.int32(first), None)

        def step(g, carry):
            stage(c, g, g - 1)
            return carry

        lax.fori_loop(first + 1, end, step, 0)
        stage(c, None, jnp.int32(end - 1))
        rows = slice(c * rows_c, (c + 1) * rows_c)
        a = abuf[rows, :]
        for i in range(0, width, 512):
            parts[1, rows, i:i + 512] = dot(a, wout[:, i:i + 512]).astype(BF16)

    def update(count):
        lo = done[0]
        done[0] += count

        def group(g, carry):
            base = g * GROUP
            page = lax.div(g, groups_c)
            turn = 128 - lax.rem(g, groups_c) * GROUP
            k_cols = pltpu.roll(kcols[page].astype(F32), turn, 1)
            v_cols = pltpu.roll(vcols[page].astype(F32), turn, 1)
            for b in range(GROUP):
                here = lane16 == jnp.full((16, slots), lens[base + b].astype(F32), F32).astype(BF16)
                for cols, ref in ((k_cols, keys), (v_cols, values)):
                    column = jnp.broadcast_to(cols[:, b:b + 1], (hd, slots)).astype(BF16).reshape(hd // 16, 16, slots)
                    old = ref[base + b].reshape(hd // 16, 16, slots)
                    ref[base + b] = jnp.where(here[None], column, old).reshape(hd, slots)
            return carry

        lax.fori_loop(lo, lo + count, group, 0)

    done = [0]

    x_copies = [pltpu.make_async_copy(x_hbm.at[rows_of(c, me)], xown.at[c], w_sem.at[c]) for c in range(CHUNKS)]
    up_copies = [[pltpu.make_async_copy(wup_hbm.at[l], wup, w_sem.at[2 + 2 * l]),
                  pltpu.make_async_copy(wdown_hbm.at[l], wdown, w_sem.at[3 + 2 * l])] for l in range(2)]
    qkv_copies = [pltpu.make_async_copy(wqkv_hbm.at[1], wqkv, w_sem.at[6]), pltpu.make_async_copy(wout_hbm.at[1], wout, w_sem.at[7])]
    piece = batch // PIECES
    caches = []
    for p in range(PIECES):
        rows = slice(p * piece, (p + 1) * piece)
        caches.append(pltpu.make_async_copy(k_hbm.at[1, rows], keys.at[rows], cache_sem.at[0, p]))
        caches.append(pltpu.make_async_copy(v_hbm.at[1, rows], values.at[rows], cache_sem.at[1, p]))
    pending = list(caches)

    def start_caches(count):
        for copy in pending[:count]:
            copy.start()
        del pending[:count]

    results = []
    for c in range(CHUNKS):
        rows = slice(c * rows_c, (c + 1) * rows_c)
        results.append(pltpu.make_async_copy(hbuf.at[3, rows], full_ref.at[rows], w_sem.at[8 + c]))

    def run(copies, wait):
        for copy in copies:
            if wait:
                copy.wait()
            else:
                copy.start()

    barrier = pltpu.get_barrier_semaphore()
    for peer in (partner,) + tuple(t * 2 + core for t in chips[:3]):
        pl.semaphore_signal(barrier, inc=1, device_id={"tp": peer}, device_id_type=MESH)
    pl.semaphore_wait(barrier, 4)

    send_pairs(0, 0)
    send_pairs(0, 1)
    run(x_copies, False)
    run(up_copies[0], False)
    run(qkv_copies, False)
    add_pairs(0, 0)
    add_pairs(0, 1)
    start_caches(2)
    run(x_copies, True)
    finish(0, 0)
    start_caches(2)
    finish(0, 1)
    start_caches(2)
    run(up_copies[0], True)
    forward(0, 0)
    start_caches(1)
    arrived(0, 0)
    mlp(0, 0)
    send_pairs(1, 0)
    forward(0, 1)
    add_pairs(1, 0)
    start_caches(1)
    arrived(0, 1)
    mlp(0, 1)
    send_pairs(1, 1)
    start_caches(2)
    add_pairs(1, 1)
    run(up_copies[1], False)
    start_caches(2)
    finish(1, 0)
    start_caches(2)
    finish(1, 1)
    start_caches(2)
    run(qkv_copies, True)
    forward(1, 0)
    arrived(1, 0)
    project(0)
    forward(1, 1)
    run(caches, True)
    attend(0)
    send_pairs(2, 0)
    arrived(1, 1)
    project(1)
    add_pairs(2, 0)
    attend(1)
    send_pairs(2, 1)
    finish(2, 0)
    add_pairs(2, 1)
    update(UPDATES[0])
    finish(2, 1)
    run(up_copies[1], True)
    update(UPDATES[1])
    forward(2, 0)
    arrived(2, 0)
    mlp(1, 0)
    send_pairs(3, 0)
    forward(2, 1)
    add_pairs(3, 0)
    arrived(2, 1)
    mlp(1, 1)
    send_pairs(3, 1)
    update(UPDATES[2])
    add_pairs(3, 1)
    update(UPDATES[3])
    finish(3, 0)
    update(UPDATES[4])
    finish(3, 1)
    update(UPDATES[5])
    forward(3, 0)
    update(UPDATES[6])
    forward(3, 1)
    for c in range(CHUNKS):
        arrived(3, c)
        results[c].start()
    run(results, True)
    for s in range(4):
        for c in range(CHUNKS):
            for k in range(4):
                pair_copy(s, c, k).wait_send()
                gather_copy(s, c, k).wait_send()
                if k < 3:
                    if s > 1:
                        cross_copy(s, c, k).wait_send()
                    forward_copy(s, c, k).wait_send()


def middle(lens, part, x, gains, biases, bqkv, bout, bup, bdown, wqkv, wout, wup, wdown, k_in, v_in):
    batch, width = part.shape
    hidden = wup.shape[2]
    hd, slots = k_in.shape[2:]
    rows_o = batch // CHUNKS // 8
    any_spec = pl.BlockSpec(memory_space=pl.ANY)
    vmem_spec = pl.BlockSpec(memory_space=pltpu.VMEM)
    own = (CHUNKS, rows_o, width)
    dma = pltpu.SemaphoreType.DMA
    return pl.pallas_call(
        middle_kernel,
        out_shape=(jax.ShapeDtypeStruct((batch, width), BF16), pltpu.VMEM(k_in.shape[1:], BF16), pltpu.VMEM(v_in.shape[1:], BF16)),
        in_specs=[pl.BlockSpec(memory_space=pltpu.SMEM), vmem_spec, any_spec] + [vmem_spec] * 6 + [any_spec] * 6,
        out_specs=(any_spec, vmem_spec, vmem_spec),
        scratch_shapes=[
            pltpu.VMEM((3 * hd, width), BF16),
            pltpu.VMEM((hd, width), BF16),
            pltpu.VMEM((width, hidden), BF16),
            pltpu.VMEM((hidden, width), BF16),
            pltpu.VMEM((3, batch, width), BF16),
            pltpu.VMEM((4, batch, width), BF16),
            pltpu.VMEM((batch // CHUNKS, hidden), BF16),
            pltpu.VMEM((2, CHUNKS, 4, rows_o, width), BF16),
            pltpu.VMEM((2, CHUNKS, 3, rows_o, width), BF16),
            pltpu.VMEM((2, CHUNKS, 3, rows_o, width), BF16),
            pltpu.VMEM(own, F32),
            pltpu.VMEM(own, BF16),
            pltpu.VMEM((batch * 4, hd), BF16),
            pltpu.VMEM((CHUNKS, hd, 128), BF16),
            pltpu.VMEM((CHUNKS, hd, 128), BF16),
            pltpu.VMEM((batch, hd), BF16),
            pltpu.VMEM((2, GROUP * 4, slots), F32),
            pltpu.VMEM((batch, hd), BF16),
            dma((8 + CHUNKS,)),
            dma((2, PIECES)),
            dma((4, CHUNKS, 4)),
            dma((4, CHUNKS, 4)),
            dma((4, CHUNKS, 3)),
            dma((4, CHUNKS, 3)),
            dma((4, CHUNKS, 4)),
            dma((4, CHUNKS, 4)),
            dma((4, CHUNKS, 3)),
            dma((4, CHUNKS, 3)),
        ],
        compiler_params=pltpu.CompilerParams(
            collective_id=0, has_side_effects=True, vmem_limit_bytes=25 * 1024 * 1024),
        name="middle",
    )(lens, part, x, gains, biases, bqkv, bout, bup, bdown, wqkv, wout, wup, wdown, k_in, v_in)


def write_kernel(x_ref, keys, values, k_old, v_old, x_out, k_out, v_out, sem):
    piece = keys.shape[0] // PIECES
    copies = []
    for p in range(PIECES):
        rows = slice(p * piece, (p + 1) * piece)
        copies.append(pltpu.make_async_copy(keys.at[rows], k_out.at[1, rows], sem.at[0, p]))
        copies.append(pltpu.make_async_copy(values.at[rows], v_out.at[1, rows], sem.at[1, p]))
    for copy in copies:
        copy.start()
    x_out[...] = x_ref[...]
    for copy in copies:
        copy.wait()


def write(x, keys, values, k_out, v_out):
    any_spec = pl.BlockSpec(memory_space=pl.ANY)
    vmem_spec = pl.BlockSpec(memory_space=pltpu.VMEM)
    return pl.pallas_call(
        write_kernel,
        out_shape=(jax.ShapeDtypeStruct(x.shape, BF16), jax.ShapeDtypeStruct(k_out.shape, BF16), jax.ShapeDtypeStruct(v_out.shape, BF16)),
        in_specs=[vmem_spec] * 3 + [any_spec] * 2,
        out_specs=(vmem_spec, any_spec, any_spec),
        input_output_aliases={3: 1, 4: 2},
        scratch_shapes=[pltpu.SemaphoreType.DMA((2, PIECES))],
        compiler_params=pltpu.CompilerParams(vmem_limit_bytes=25 * 1024 * 1024),
        name="write",
    )(x, in_vmem(keys), in_vmem(values), k_out, v_out)


def in_vmem(array):
    return pltpu.with_memory_space_constraint(array, pltpu.VMEM)


def solution(mesh):
    cache_spec = P(None, 'dp', 'tp', None, None)
    in_specs = (P('dp', None), P('dp'), cache_spec, cache_spec, P(), P(),
                P(None, None, None, 'tp', None), P(None, None, 'tp', None),
                P(None, 'tp', None, None), P(), P(None, None, 'tp'), P(None, 'tp'),
                P(None, 'tp', None), P())
    out_specs = (P('dp', None), cache_spec, cache_spec)

    def local_step(x, cache_len, k_cache, v_cache, norm_gain, norm_bias, w_qkv, b_qkv, w_out, b_out, w_up, b_up, w_down, b_down):
        layers, batch, heads, slots, head = k_cache.shape
        width = x.shape[1]
        hd = heads * head
        k_in = jnp.swapaxes(k_cache, 3, 4).reshape(layers, batch, hd, slots)
        v_in = jnp.swapaxes(v_cache, 3, 4).reshape(layers, batch, hd, slots)
        wqkv = jnp.transpose(w_qkv, (0, 2, 3, 4, 1)).reshape(layers, 3 * hd, width)
        wout = w_out.reshape(layers, hd, width)

        k_out, v_out, part = attention(0, True, cache_len, x, norm_gain, norm_bias, b_qkv, wqkv, wout, k_in, v_in)
        rows, keys, values = middle(cache_len, part, x, norm_gain, norm_bias, b_qkv, b_out, b_up, b_down, wqkv, wout, w_up, w_down, k_in, v_in)
        rows, k_out, v_out = write(rows, keys, values, k_out, v_out)

        def back(cache):
            return jnp.swapaxes(cache.reshape(layers, batch, heads, head, slots), 3, 4)

        return rows, back(k_out), back(v_out)

    return jax.shard_map(local_step, mesh=mesh, in_specs=in_specs, out_specs=out_specs, check_vma=False)
```
